32 devices in a mesh: lat: 16 (over z, y, x), fld: 2 (over core).
Axes of the slice: x: 2, y: 2, z: 4, core: 2. Of those that a mesh axis runs over, the one named last changes fastest.
Arguments:
- grid: bfloat16 [2, 4, 69, 640, 1408], P('fld', None, None, 'lat'), may hold values from -6 to 6
- cycle_ids: int32 [640], replicated, may hold values from 0 to 639, each once
- cycle_len: int32 [640], replicated, may hold values from 20 to 1296, as said below
- wave_ids: int32 [320], replicated, may hold values from 0 to 319, each once
- legendre: bfloat16 [320, 320, 640], P('lat'), may hold values from -0.25 to 0.25
- target: float32 [2, 4, 69, 2, 320, 320], P('fld', None, None, None, 'lat'), may hold values from -18 to 18
- step_w: float32 [2], P('fld'), may hold values from 0.5 to 2
- chan_w: float32 [69], replicated, may hold values from 0.2 to 2
Outputs:
- coeffs: float32 [2, 4, 69, 2, 320, 320], P('fld', None, None, None, 'lat')
- loss: float32 [], replicated
- field_grad: bfloat16 [2, 4, 69, 640, 1408], P('fld', None, None, 'lat')
The draws below stay inside these ranges and needn't reach their ends.
Inputs may be any that keep to these rules, and one draw needn't show every extreme that they name: `cycle_len`: every length 20 + 4 j with j from 0 to 319 occurs exactly twice.
All inputs are finite; a program needn't handle non-finite values.
Results may differ from the reference program's by a relative error of at most 0.0065.
Values may be sent and summed in bfloat16 or wider, within the bound.
No kernel may reach another device: no remote copies, remote signals or barrier semaphores. Data moves between devices by JAX's collectives and lax.ppermute only.
A program may use at most 320 MiB of HBM per device.

```python
import math
import jax
import jax.numpy as jnp
from jax import lax

R = 640
MW = 320
CH = 69
BATCH = 4
STEPS = 2
SEG = 1408


def draw_cycle_len(key, part):
    order = jax.random.permutation(jax.random.fold_in(key, 11), R).astype(jnp.int32)
    return (20 + 4 * (order // 2)).astype(jnp.int32)


def draw_target(key, part):
    shape = (STEPS, BATCH, CH, 2, MW, MW)
    slot_index = jnp.arange(MW, dtype=jnp.float32) / (MW - 1)
    values = jnp.clip(jax.random.normal(jax.random.fold_in(key, 22), shape, jnp.float32), -6.0, 6.0)
    slot_scale = 0.5 + 2.5 * slot_index
    return (values * slot_scale[:, None]).astype(jnp.float32)


def steps_of(rng, extent, cuts, least, top_value):
    factor_of, own = 1.0, jax.random.fold_in(rng, 6)
    for axis_at, parts in cuts:
        draws = jnp.exp(jax.random.uniform(jax.random.fold_in(own, axis_at), (parts,), jnp.float32, least / len(cuts), top_value / len(cuts)))
        factor_of = factor_of * jnp.repeat(draws, extent[axis_at] // parts).reshape([-1 if axis == axis_at else 1 for axis in range(len(extent))])
    return factor_of


def scatter_about(rng, dims, spread, bound, shards=(), kind=jnp.bfloat16):
    gain = steps_of(rng, dims, shards, -0.22, 0.18) if shards else 1.0
    result = jax.random.normal(rng, dims, jnp.float32) * spread * gain
    return jnp.minimum(jnp.maximum(result, -bound), bound).astype(kind)


def setup_inputs(seed: int = 0) -> dict:
    keys = jax.random.split(jax.random.key(seed), 9)
    return {
        "grid": scatter_about(keys[0], (STEPS, BATCH, CH, R, SEG), 1.0, 6.0, ((0, 2), (3, 16))),
        "cycle_ids": jax.random.permutation(keys[1], R).astype(jnp.int32),
        "cycle_len": draw_cycle_len(jax.random.fold_in(keys[8], 71), 0),
        "wave_ids": jax.random.permutation(keys[3], MW).astype(jnp.int32),
        "legendre": scatter_about(keys[4], (MW, MW, R), R ** -0.5, 0.25, ((0, 16),)),
        "target": draw_target(jax.random.fold_in(keys[8], 71), 0),
        "step_w": jnp.clip(jnp.exp(math.log(2.0) - 1.3862944 * jax.random.uniform(keys[6], (STEPS,), jnp.float32) ** steps_of(keys[6], (STEPS,), ((0, 2),), -0.2, 0.2)), 0.5, 2.0),
        "chan_w": jnp.clip(jnp.exp(jax.random.uniform(keys[7], (CH,), jnp.float32, math.log(0.2), math.log(2.0))), 0.2, 2.0),
    }


def cycle_table(length, wave_order, segment):
    slot_index = jnp.arange(segment, dtype=jnp.int32)
    phase_int = slot_index[:, None] * wave_order[None, :] % length
    angles = 2.0 * math.pi / length.astype(jnp.float32) * phase_int.astype(jnp.float32)
    inside = (slot_index[:, None] < length) & (2 * wave_order[None, :] < length)
    row_scale = jnp.where(inside, lax.rsqrt(length.astype(jnp.float32)), jnp.float32(0.0))
    paired = jnp.stack([jnp.cos(angles) * row_scale, -jnp.sin(angles) * row_scale], axis=2)
    return paired.reshape(segment, 2 * wave_order.shape[0]).astype(jnp.bfloat16)

def reference(grid, cycle_ids, cycle_len, wave_ids, legendre, target, step_w, chan_w):
    step_count, batch_size, chan_count, cycle_count, segment = grid.shape
    wave_count = wave_ids.shape[0]
    col_count = step_count * batch_size * chan_count
    highest = lax.Precision.HIGHEST

    def forward_cycle(cycle_slot):
        length = cycle_len[cycle_ids[cycle_slot]]
        dft_table = cycle_table(length, wave_ids, segment).astype(jnp.float32)
        grid_rows = lax.dynamic_index_in_dim(grid, cycle_slot, 3, keepdims=False)
        grid_rows = grid_rows.reshape(col_count, segment).astype(jnp.float32)
        return jnp.dot(grid_rows, dft_table, precision=highest).astype(jnp.bfloat16)
    fourier = lax.map(forward_cycle, jnp.arange(cycle_count, dtype=jnp.int32))
    fourier = fourier.reshape(cycle_count, col_count, wave_count, 2)
    basis_all = jnp.take(legendre, cycle_ids, axis=2)
    degree = jnp.arange(wave_count, dtype=jnp.int32)
    weight_cols = jnp.broadcast_to(step_w[:, None, None] * chan_w[None, None, :], (step_count, batch_size, chan_count)).reshape(col_count)

    def per_slot(wave_slot):
        basis = lax.dynamic_index_in_dim(basis_all, wave_slot, 0, keepdims=False).astype(jnp.float32)
        slot_fourier = lax.dynamic_index_in_dim(fourier, wave_slot, 2, keepdims=False)
        slot_fourier = slot_fourier.astype(jnp.float32).reshape(cycle_count, col_count * 2)
        coeffs = jnp.dot(basis, slot_fourier, precision=highest).reshape(wave_count, col_count, 2)
        wave_num = wave_ids[wave_slot]
        kept_mask = (degree >= wave_num).astype(jnp.float32)[:, None, None]
        coeffs = coeffs * kept_mask
        target_slot = lax.dynamic_index_in_dim(target, wave_slot, 4, keepdims=False)
        target_slot = jnp.transpose(target_slot.reshape(col_count, 2, wave_count), (2, 0, 1))
        factor = jnp.where(wave_num == 0, 1.0, 2.0).astype(jnp.float32)
        weight = (factor * weight_cols)[None, :, None]
        misfit = (coeffs - target_slot) * kept_mask
        partial_value = jnp.sum(weight * misfit * misfit)
        grad_coeff = (2.0 * weight * misfit).astype(jnp.bfloat16)
        back_rows = jnp.dot(basis.T, grad_coeff.astype(jnp.float32).reshape(wave_count, col_count * 2), precision=highest).astype(jnp.bfloat16)
        return (jnp.transpose(coeffs, (1, 2, 0)), partial_value, back_rows.reshape(cycle_count, col_count, 2))
    coeff_all, partials, back_all = lax.map(per_slot, jnp.arange(wave_count, dtype=jnp.int32))
    coeff_all = coeff_all.reshape(wave_count, step_count, batch_size, chan_count, 2, wave_count)
    coeffs = jnp.moveaxis(coeff_all, 0, 4)

    def adjoint_cycle(cycle_slot):
        length = cycle_len[cycle_ids[cycle_slot]]
        dft_table = cycle_table(length, wave_ids, segment).astype(jnp.float32)
        slot_back = lax.dynamic_index_in_dim(back_all, cycle_slot, 1, keepdims=False)
        slot_back = jnp.transpose(slot_back, (1, 0, 2)).reshape(col_count, 2 * wave_count)
        return jnp.dot(slot_back.astype(jnp.float32), dft_table.T, precision=highest).astype(jnp.bfloat16)
    field_rows = lax.map(adjoint_cycle, jnp.arange(cycle_count, dtype=jnp.int32))
    field_rows = field_rows.reshape(cycle_count, step_count, batch_size, chan_count, segment)
    field_grad = jnp.moveaxis(field_rows, 0, 3)
    term_count = step_count * batch_size * chan_count * wave_count * (wave_count + 1) // 2
    loss = jnp.sum(partials) / jnp.float32(term_count)
    return (coeffs, loss, field_grad)
```

```python
import functools
import math

import jax
import jax.numpy as jnp
from jax import lax
from jax.experimental import pallas as pl
from jax.experimental.pallas import tpu as pltpu
from jax.sharding import PartitionSpec as P

STEPS = 2
KB = 256
GROUP = 8
LANES = 128


def round_up(value, unit):
    return (value + unit - 1) // unit * unit


def phasor_rows(lengths, wave_ids, block_count, wave_pad):
    exponents = [1 << bit for bit in range(8)] + [KB * block for block in range(block_count)]
    exponents = jnp.asarray(exponents, dtype=jnp.int32)
    length = lengths[:, None, None]
    phase = (exponents[None, :, None] * wave_ids[None, None, :]) % length
    length_f = length.astype(jnp.float32)
    turn = phase.astype(jnp.float32) / length_f
    quarter = jnp.floor(turn * 4.0 + 0.5)
    x = (turn - 0.25 * quarter) * jnp.float32(2.0 * math.pi)
    x2 = x * x
    sin_x = x * (1.0 + x2 * (-1.0 / 6 + x2 * (1.0 / 120 + x2 * (-1.0 / 5040 + x2 * (1.0 / 362880)))))
    cos_x = 1.0 + x2 * (
        -0.5 + x2 * (1.0 / 24 + x2 * (-1.0 / 720 + x2 * (1.0 / 40320 + x2 * (-1.0 / 3628800))))
    )
    odd = (quarter == 1.0) | (quarter == 3.0)
    cos_t = jnp.where(odd, sin_x, cos_x)
    cos_t = jnp.where((quarter == 1.0) | (quarter == 2.0), -cos_t, cos_t)
    sin_t = jnp.where(odd, cos_x, sin_x)
    sin_t = jnp.where((quarter == 2.0) | (quarter == 3.0), -sin_t, sin_t)
    scale = jnp.where(2 * wave_ids[None, None, :] < length, lax.rsqrt(length_f), jnp.float32(0.0))
    lane_pad = ((0, 0), (0, 0), (0, wave_pad - wave_ids.shape[0]))
    cos_t = jnp.concatenate([cos_t, scale], axis=1)
    sin_t = jnp.concatenate([-sin_t, jnp.zeros_like(scale)], axis=1)
    rows = jnp.concatenate([jnp.pad(cos_t, lane_pad), jnp.pad(sin_t, lane_pad)], axis=2)
    row_pad = round_up(rows.shape[1], 8) - rows.shape[1]
    return jnp.pad(rows, ((0, 0), (0, row_pad), (0, 0)))


def rotate(cos_a, sin_a, cos_b, sin_b):
    return cos_a * cos_b - sin_a * sin_b, cos_a * sin_b + sin_a * cos_b


def build_base(ph_ref, base_ref, slot, wave_pad, scale_row):
    row = lax.broadcasted_iota(jnp.int32, (8, wave_pad), 0)
    cos_v = jnp.broadcast_to(ph_ref[slot, scale_row : scale_row + 1, :wave_pad], (8, wave_pad))
    sin_v = jnp.zeros((8, wave_pad), jnp.float32)
    for bit in range(3):
        on = ((row >> bit) & 1) == 1
        cos_b = jnp.where(on, ph_ref[slot, bit : bit + 1, :wave_pad], 1.0)
        sin_b = jnp.where(on, ph_ref[slot, bit : bit + 1, wave_pad:], 0.0)
        cos_v, sin_v = rotate(cos_v, sin_v, cos_b, sin_b)
    base_ref[0:8, :wave_pad] = cos_v
    base_ref[0:8, wave_pad:] = sin_v
    size, bit = 8, 3
    while size < KB:
        cos_b = ph_ref[slot, bit : bit + 1, :wave_pad]
        sin_b = ph_ref[slot, bit : bit + 1, wave_pad:]
        for start in range(0, size, 32):
            stop = min(start + 32, size)
            cos_v, sin_v = rotate(
                base_ref[start:stop, :wave_pad], base_ref[start:stop, wave_pad:], cos_b, sin_b
            )
            base_ref[size + start : size + stop, :wave_pad] = cos_v
            base_ref[size + start : size + stop, wave_pad:] = sin_v
        size, bit = size * 2, bit + 1


def table_block(ph_ref, base_ref, table_ref, slot, block, wave_pad):
    turn = ph_ref[slot, pl.ds(8 + block, 1), :]
    cos_b, sin_b = turn[:, :wave_pad], turn[:, wave_pad:]
    for start in range(0, KB, 32):
        stop = start + 32
        cos_v, sin_v = rotate(
            base_ref[start:stop, :wave_pad], base_ref[start:stop, wave_pad:], cos_b, sin_b
        )
        table_ref[start:stop, :wave_pad] = cos_v.astype(jnp.bfloat16)
        table_ref[start:stop, wave_pad:] = sin_v.astype(jnp.bfloat16)


def forward_kernel(
    wave_count, wave_pad, scale_row, groups, rest, len_ref, ph_ref, *refs
):
    if rest:
        grid_ref, grid_rest_ref, out_ref, base_ref, table_ref, wide_ref, acc_ref, rows_ref, wide_rest_ref, rest_ref = refs
        rest_cols = grid_rest_ref.shape[0]
        per_row = LANES // rest
        rest_rows = rest_ref.shape[0] // (2 * wave_count)
    else:
        grid_ref, out_ref, base_ref, table_ref, wide_ref, acc_ref, rows_ref = refs
        rest_cols = 0
    group = pl.program_id(0)
    segment = grid_ref.shape[2]
    owners, _, wave_dev = out_ref.shape[:3]

    def store_rows(source):
        for part in range(2):
            rows = source[part * wave_count * GROUP : (part + 1) * wave_count * GROUP, :]
            out_ref[:, part] = rows.reshape(owners, wave_dev, GROUP, LANES).astype(jnp.bfloat16)

    def run_group():
        for lane in range(segment // LANES):
            piece = grid_ref[:, :, lane * LANES : (lane + 1) * LANES].astype(jnp.float32)
            wide_ref[lane] = piece.reshape(LANES * GROUP, LANES)
            if rest:
                piece = grid_rest_ref[:, :, lane * LANES : (lane + 1) * LANES].astype(jnp.float32)
                wide_rest_ref[lane] = piece.reshape(rest_cols * GROUP, LANES)

        def per_slot(slot, carry):
            length = len_ref[group * GROUP + slot]
            build_base(ph_ref, base_ref, slot, wave_pad, scale_row)
            acc_ref[...] = jnp.zeros_like(acc_ref)

            def per_block(block, inner):
                table_block(ph_ref, base_ref, table_ref, slot, block, wave_pad)
                pieces = []
                for part in range(KB // LANES):
                    lane_block = block * (KB // LANES) + part
                    values = wide_ref[lane_block, pl.ds(slot, LANES, stride=GROUP), :]
                    if rest:
                        extra = wide_rest_ref[lane_block, pl.ds(slot, rest_cols, stride=GROUP), :]
                        values = jnp.concatenate([values, extra], axis=0)
                    at = lane_block * LANES + lax.broadcasted_iota(jnp.int32, values.shape, 1)
                    pieces.append(jnp.where(at < length, values, 0.0).astype(jnp.bfloat16))
                acc_ref[...] += jnp.dot(
                    jnp.concatenate(pieces, axis=1), table_ref[...], preferred_element_type=jnp.float32
                )
                return inner

            lax.fori_loop(0, (length + KB - 1) // KB, per_block, 0)
            for part in range(2):
                lanes = slice(part * wave_pad, (part + 1) * wave_pad)
                turned = acc_ref[:LANES, lanes].T
                rows_ref[pl.ds(part * wave_count * GROUP + slot, wave_count, stride=GROUP), :] = (
                    turned[:wave_count]
                )
                if rest:
                    cycle = group * GROUP + slot
                    turned = acc_ref[LANES:, lanes].T[:wave_count]
                    fill = jnp.zeros((wave_count, LANES - rest_cols), jnp.float32)
                    turned = jnp.concatenate([turned, fill], axis=1)
                    keep = lax.broadcasted_iota(jnp.int32, turned.shape, 1) < rest
                    turned = jnp.where(keep, turned, 0.0)
                    turned = pltpu.roll(turned, lax.rem(cycle, per_row) * rest, 1)
                    at = pl.ds(part * wave_count * rest_rows + cycle // per_row, wave_count, stride=rest_rows)
                    rest_ref[at, :] += turned
            return carry

        lax.fori_loop(0, GROUP, per_slot, 0)
        store_rows(rows_ref)

    if rest:

        @pl.when(group == 0)
        def _():
            rest_ref[...] = jnp.zeros_like(rest_ref)

        pl.when(group < groups)(run_group)

        @pl.when(group == groups)
        def _():
            store_rows(rest_ref)
    else:
        run_group()


def forward_dft(grid, lengths, phasors, owners, wave_count, wave_pad, scale_row, chunk):
    index, rest, rest_cols, rest_index = chunk
    col_count, cycle_dev, segment = grid.shape
    groups = pl.cdiv(cycle_dev, GROUP)
    wide_lanes = round_up(segment, KB) // LANES
    wave_dev = wave_count // owners
    rows = (groups + (1 if rest else 0)) * GROUP
    last = groups - 1
    in_specs = [
        pl.BlockSpec((GROUP,) + phasors.shape[1:], lambda g, n: (jnp.minimum(g, last), 0, 0)),
        pl.BlockSpec((LANES, GROUP, segment), lambda g, n: (index, jnp.minimum(g, last), 0)),
    ]
    operands = [lengths, phasors, grid]
    scratch = [
        pltpu.VMEM((KB, 2 * wave_pad), jnp.float32),
        pltpu.VMEM((KB, 2 * wave_pad), jnp.bfloat16),
        pltpu.VMEM((wide_lanes, LANES * GROUP, LANES), jnp.float32),
        pltpu.VMEM((LANES + rest_cols, 2 * wave_pad), jnp.float32),
        pltpu.VMEM((2 * wave_count * GROUP, LANES), jnp.float32),
    ]
    if rest:
        in_specs.append(
            pl.BlockSpec((rest_cols, GROUP, segment), lambda g, n: (rest_index, jnp.minimum(g, last), 0))
        )
        operands.append(grid)
        scratch += [
            pltpu.VMEM((wide_lanes, rest_cols * GROUP, LANES), jnp.float32),
            pltpu.VMEM((2 * wave_count * GROUP, LANES), jnp.float32),
        ]
    return pl.pallas_call(
        functools.partial(forward_kernel, wave_count, wave_pad, scale_row, groups, rest),
        out_shape=jax.ShapeDtypeStruct((owners, 2, wave_dev, rows, LANES), jnp.bfloat16),
        grid_spec=pltpu.PrefetchScalarGridSpec(
            num_scalar_prefetch=1,
            grid=(rows // GROUP,),
            in_specs=in_specs,
            out_specs=pl.BlockSpec((owners, 2, wave_dev, GROUP, LANES), lambda g, n: (0, 0, 0, g, 0)),
            scratch_shapes=scratch,
        ),
        compiler_params=pltpu.CompilerParams(
            dimension_semantics=("arbitrary",), vmem_limit_bytes=56 * 1024 * 1024
        ),
        cost_estimate=pl.CostEstimate(
            flops=2 * LANES * cycle_dev * segment * wave_pad,
            bytes_accessed=2 * LANES * cycle_dev * (segment + 2 * wave_count),
            transcendentals=0,
        ),
        name="forward_dft",
    )(*operands)


def adjoint_kernel(wave_count, wave_pad, scale_row, rest, aliased, len_ref, ph_ref, *refs):
    refs = list(refs)
    back_ref = refs.pop(0)
    back_rest_ref = refs.pop(0) if rest else None
    if aliased:
        refs.pop(0)
    out_ref = refs.pop(0)
    out_rest_ref = refs.pop(0) if rest else None
    base_ref, table_ref, lhs_ref, rows_ref, wide_ref = refs[:5]
    if rest:
        wide_rest_ref, rest_ref = refs[5:]
        rest_cols = out_rest_ref.shape[0]
        per_row = LANES // rest
    group = pl.program_id(0)
    segment = out_ref.shape[2]
    lane_count = wide_ref.shape[0]
    per_kb = KB // LANES
    span = wave_count * GROUP
    for part in range(2):
        rows_ref[part * span : (part + 1) * span, :] = (
            back_ref[:, part].astype(jnp.float32).reshape(span, LANES)
        )

    @pl.when(group == 0)
    def _():
        lhs_ref[...] = jnp.zeros_like(lhs_ref)
        if rest:
            for part in range(2):
                rest_ref[part * span : (part + 1) * span, :] = (
                    back_rest_ref[:, part].astype(jnp.float32).reshape(span, LANES)
                )

    def put(slot, lane_block, values):
        wide_ref[lane_block, pl.ds(slot, LANES, stride=GROUP), :] = values[:LANES]
        if rest:
            wide_rest_ref[lane_block, pl.ds(slot, rest_cols, stride=GROUP), :] = values[LANES:]

    def per_slot(slot, carry):
        length = len_ref[group * GROUP + slot]
        build_base(ph_ref, base_ref, slot, wave_pad, scale_row)
        for part in range(2):
            lanes = slice(part * wave_pad, part * wave_pad + wave_count)
            turned = rows_ref[pl.ds(part * span + slot, wave_count, stride=GROUP), :].T
            lhs_ref[:LANES, lanes] = turned.astype(jnp.bfloat16)
            if rest:
                cycle = group * GROUP + slot
                rows = rest_ref[pl.ds(part * span + cycle // per_row, wave_count, stride=GROUP), :]
                rows = pltpu.roll(rows, LANES - lax.rem(cycle, per_row) * rest, 1)
                lhs_ref[LANES:, lanes] = rows[:, :rest_cols].T.astype(jnp.bfloat16)
        used = (length + KB - 1) // KB

        def per_block(block, inner):
            table_block(ph_ref, base_ref, table_ref, slot, block, wave_pad)
            values = lax.dot_general(
                lhs_ref[...], table_ref[...], (((1,), (1,)), ((), ())), preferred_element_type=jnp.float32
            )
            for part in range(per_kb):
                lane_block = block * per_kb + part
                piece = values[:, part * LANES : (part + 1) * LANES]
                at = lane_block * LANES + lax.broadcasted_iota(jnp.int32, piece.shape, 1)
                put(slot, lane_block, jnp.where(at < length, piece, 0.0))
            return inner

        def fill(lane_block, inner):
            put(slot, lane_block, jnp.zeros((lhs_ref.shape[0], LANES), jnp.float32))
            return inner

        lax.fori_loop(0, used, per_block, 0)
        lax.fori_loop(used * per_kb, lane_count, fill, 0)
        return carry

    lax.fori_loop(0, GROUP, per_slot, 0)
    for lane in range(segment // LANES):
        lanes = slice(lane * LANES, (lane + 1) * LANES)
        out_ref[:, :, lanes] = wide_ref[lane].reshape(LANES, GROUP, LANES).astype(jnp.bfloat16)
        if rest:
            values = wide_rest_ref[lane].reshape(rest_cols, GROUP, LANES)
            out_rest_ref[:, :, lanes] = values.astype(jnp.bfloat16)


def adjoint_dft(back, field, lengths, phasors, out_shape, wave_count, wave_pad, scale_row, chunk):
    index, rest, rest_cols, rest_index = chunk
    col_count, cycle_dev, segment = out_shape
    owners, _, wave_dev, rows, _ = back.shape
    groups = pl.cdiv(cycle_dev, GROUP)
    wide_lanes = round_up(segment, KB) // LANES
    aliased = field is not None
    block = (owners, 2, wave_dev, GROUP, LANES)
    in_specs = [
        pl.BlockSpec((GROUP,) + phasors.shape[1:], lambda g, n: (g, 0, 0)),
        pl.BlockSpec(block, lambda g, n: (0, 0, 0, g, 0)),
    ]
    operands = [lengths, phasors, back]
    out_specs = [pl.BlockSpec((LANES, GROUP, segment), lambda g, n: (index, g, 0))]
    out_shapes = [jax.ShapeDtypeStruct(out_shape, jnp.bfloat16)]
    scratch = [
        pltpu.VMEM((KB, 2 * wave_pad), jnp.float32),
        pltpu.VMEM((KB, 2 * wave_pad), jnp.bfloat16),
        pltpu.VMEM((LANES + rest_cols, 2 * wave_pad), jnp.bfloat16),
        pltpu.VMEM((2 * wave_count * GROUP, LANES), jnp.float32),
        pltpu.VMEM((wide_lanes, LANES * GROUP, LANES), jnp.float32),
    ]
    if rest:
        in_specs.append(pl.BlockSpec(block, lambda g, n: (0, 0, 0, groups, 0)))
        operands.append(back)
        out_specs.append(pl.BlockSpec((rest_cols, GROUP, segment), lambda g, n: (0, g, 0)))
        out_shapes.append(jax.ShapeDtypeStruct((rest_cols, cycle_dev, segment), jnp.bfloat16))
        scratch += [
            pltpu.VMEM((wide_lanes, rest_cols * GROUP, LANES), jnp.float32),
            pltpu.VMEM((2 * wave_count * GROUP, LANES), jnp.float32),
        ]
    aliases = {}
    if aliased:
        aliases = {len(operands): 0}
        in_specs.append(pl.BlockSpec(memory_space=pl.ANY))
        operands.append(field)
    return pl.pallas_call(
        functools.partial(adjoint_kernel, wave_count, wave_pad, scale_row, rest, aliased),
        out_shape=out_shapes,
        grid_spec=pltpu.PrefetchScalarGridSpec(
            num_scalar_prefetch=1, grid=(groups,), in_specs=in_specs, out_specs=out_specs, scratch_shapes=scratch
        ),
        input_output_aliases=aliases,
        compiler_params=pltpu.CompilerParams(
            dimension_semantics=("arbitrary",), vmem_limit_bytes=60 * 1024 * 1024
        ),
        cost_estimate=pl.CostEstimate(
            flops=2 * LANES * cycle_dev * segment * wave_pad,
            bytes_accessed=2 * LANES * cycle_dev * (segment + 2 * wave_count),
            transcendentals=0,
        ),
        name="adjoint_dft",
    )(*operands)


def column_chunks(col_count):
    whole = col_count // LANES
    rest = col_count - whole * LANES
    chunks = [(index, 0, 0, 0) for index in range(whole)]
    if rest:
        width = 8
        while width < rest:
            width *= 2
        chunks[-1] = (whole - 1, rest, width, whole * LANES // width)
    return chunks


def per_device(grid, cycle_ids, cycle_len, wave_ids, legendre, target, step_w, chan_w):
    _, batch_size, chan_count, cycle_dev, segment = grid.shape
    wave_count = wave_ids.shape[0]
    wave_dev, degree_count, cycle_count = legendre.shape
    owners = wave_count // wave_dev
    col_count = batch_size * chan_count
    wave_pad = round_up(wave_count, LANES)
    block_count = pl.cdiv(segment, KB)
    scale_row = 8 + block_count
    lat_index = lax.axis_index("lat")
    my_cycles = lax.dynamic_slice_in_dim(cycle_ids, lat_index * cycle_dev, cycle_dev)
    lengths = jnp.take(cycle_len, my_cycles)
    phasors = phasor_rows(lengths, wave_ids, block_count, wave_pad)
    group_pad = round_up(cycle_dev, GROUP) - cycle_dev
    if group_pad:
        lengths = jnp.pad(lengths, (0, group_pad))
        phasors = jnp.pad(phasors, ((0, group_pad), (0, 0), (0, 0)))
    grid3 = grid.reshape(col_count, cycle_dev, segment)
    my_waves = lax.dynamic_slice_in_dim(wave_ids, lat_index * wave_dev, wave_dev)
    degree = jnp.arange(degree_count, dtype=jnp.int32)
    kept = (degree[None, :] >= my_waves[:, None]).astype(jnp.float32)[:, :, None, None]
    factor = jnp.where(my_waves == 0, 1.0, 2.0).astype(jnp.float32)
    weight_cols = jnp.broadcast_to(step_w[0] * chan_w[None, :], (batch_size, chan_count)).reshape(
        col_count
    )
    target3 = target.reshape(col_count, 2, wave_dev, degree_count)

    def exchange(values):
        shape = values.shape
        flat = values.reshape((owners * 2 * wave_dev,) + shape[3:])
        return lax.all_to_all(flat, "lat", split_axis=0, concat_axis=0, tiled=True).reshape(shape)

    chunks = column_chunks(col_count)
    groups = pl.cdiv(cycle_dev, GROUP)
    sent = []
    for chunk in chunks:
        part = forward_dft(grid3, lengths, phasors, owners, wave_count, wave_pad, scale_row, chunk)
        part, lengths, legendre, target3 = lax.optimization_barrier((part, lengths, legendre, target3))
        sent.append(part)
    legendre_cols = jnp.take(legendre, cycle_ids, axis=2).reshape(
        wave_dev, degree_count, owners, cycle_dev
    )

    def owner_pass(gathered, start, cols):
        coeffs = jnp.einsum(
            "sndp,dtspc->sntc", legendre_cols, gathered, preferred_element_type=jnp.float32
        )
        coeffs = coeffs * kept
        goal = jnp.transpose(target3[start : start + cols], (2, 3, 1, 0))
        weight = factor[:, None, None, None] * weight_cols[None, None, None, start : start + cols]
        misfit = (coeffs - goal) * kept
        value = jnp.sum(weight * misfit * misfit)
        grad_coeff = (2.0 * weight * misfit).astype(jnp.bfloat16)
        back = jnp.einsum(
            "sndp,sntc->dtspc", legendre_cols, grad_coeff, preferred_element_type=jnp.float32
        ).astype(jnp.bfloat16)
        return jnp.transpose(coeffs, (3, 2, 0, 1)), value, back

    partial_value = jnp.float32(0.0)
    coeff_parts, backs = [], []
    for chunk, part in zip(chunks, sent):
        index, rest = chunk[:2]
        gathered = exchange(part)
        coeff_part, value, back = owner_pass(gathered[:, :, :, :cycle_dev], index * LANES, LANES)
        coeff_parts.append(coeff_part)
        partial_value = partial_value + value
        row_pad = groups * GROUP - cycle_dev
        if row_pad:
            back = jnp.pad(back, ((0, 0),) * 3 + ((0, row_pad), (0, 0)))
        if rest:
            per_row = LANES // rest
            lead = gathered.shape[:3]
            packed = gathered[:, :, :, groups * GROUP :, : per_row * rest]
            unpacked = packed.reshape(lead + (GROUP * per_row, rest))[:, :, :, :cycle_dev]
            coeff_part, value, back_rest = owner_pass(unpacked, col_count - rest, rest)
            coeff_parts.append(coeff_part)
            partial_value = partial_value + value
            back_rest = jnp.pad(back_rest, ((0, 0),) * 3 + ((0, GROUP * per_row - cycle_dev), (0, 0)))
            back_rest = back_rest.reshape(lead + (GROUP, per_row * rest))
            back_rest = jnp.pad(back_rest, ((0, 0),) * 4 + ((0, LANES - per_row * rest),))
            back = jnp.concatenate([back, back_rest], axis=3)
        backs.append(back)
    loss_sum = lax.psum(partial_value, ("lat", "fld"))
    backs[-1], loss_sum = lax.optimization_barrier((backs[-1], loss_sum))
    field = None
    for chunk, back in zip(chunks, backs):
        returned = exchange(back)
        results = adjoint_dft(
            returned, field, lengths, phasors, grid3.shape, wave_count, wave_pad, scale_row, chunk
        )
        field = results[0]
        if chunk[1]:
            field = lax.dynamic_update_slice(field, results[1][: chunk[1]], (col_count - chunk[1], 0, 0))
    coeff_out = jnp.concatenate(coeff_parts, axis=0)
    term_count = STEPS * col_count * wave_count * (wave_count + 1) // 2
    loss = loss_sum / jnp.float32(term_count)
    return (
        coeff_out.reshape(1, batch_size, chan_count, 2, wave_dev, degree_count),
        loss,
        field.reshape(1, batch_size, chan_count, cycle_dev, segment),
    )


def solution(mesh):
    return jax.shard_map(
        per_device,
        mesh=mesh,
        in_specs=(
            P("fld", None, None, "lat", None),
            P(),
            P(),
            P(),
            P("lat", None, None),
            P("fld", None, None, None, "lat", None),
            P("fld"),
            P(),
        ),
        out_specs=(P("fld", None, None, None, "lat", None), P(), P("fld", None, None, "lat", None)),
        check_vma=False,
    )
```

```python
import functools
import math

import jax
import jax.numpy as jnp
from jax import lax
from jax.experimental import pallas as pl
from jax.experimental.pallas import tpu as pltpu
from jax.sharding import PartitionSpec as P


STEPS = 2
KB = 256
GROUP = 8
LANES = 128


def round_up(value, unit):
    return (value + unit - 1) // unit * unit


def phasor_rows(lengths, wave_ids, block_count, wave_pad):
    exponents = [1 << bit for bit in range(8)] + [KB * block for block in range(block_count)]
    exponents = jnp.asarray(exponents, dtype=jnp.int32)
    length = lengths[:, None, None]
    length_f = length.astype(jnp.float32)
    product = (exponents[None, :, None] * wave_ids[None, None, :]).astype(jnp.float32)
    inverse = 1.0 / length_f
    phase = product - jnp.floor(product * inverse) * length_f
    phase = jnp.where(phase < 0.0, phase + length_f, phase)
    phase = jnp.where(phase >= length_f, phase - length_f, phase)
    turn = phase * inverse
    quarter = jnp.floor(turn * 4.0 + 0.5)
    x = (turn - 0.25 * quarter) * jnp.float32(2.0 * math.pi)
    x2 = x * x
    sin_x = x * (1.0 + x2 * (-1.0 / 6 + x2 * (1.0 / 120 + x2 * (-1.0 / 5040 + x2 * (1.0 / 362880)))))
    cos_x = 1.0 + x2 * (
        -0.5 + x2 * (1.0 / 24 + x2 * (-1.0 / 720 + x2 * (1.0 / 40320 + x2 * (-1.0 / 3628800))))
    )
    odd = (quarter == 1.0) | (quarter == 3.0)
    cos_t = jnp.where(odd, sin_x, cos_x)
    cos_t = jnp.where((quarter == 1.0) | (quarter == 2.0), -cos_t, cos_t)
    sin_t = jnp.where(odd, cos_x, sin_x)
    sin_t = jnp.where((quarter == 2.0) | (quarter == 3.0), -sin_t, sin_t)
    scale = jnp.where(2 * wave_ids[None, None, :] < length, lax.rsqrt(length_f), jnp.float32(0.0))
    lane_pad = ((0, 0), (0, 0), (0, wave_pad - wave_ids.shape[0]))
    cos_t = jnp.concatenate([cos_t, scale], axis=1)
    sin_t = jnp.concatenate([-sin_t, jnp.zeros_like(scale)], axis=1)
    rows = jnp.concatenate([jnp.pad(cos_t, lane_pad), jnp.pad(sin_t, lane_pad)], axis=2)
    row_pad = round_up(rows.shape[1], 8) - rows.shape[1]
    return jnp.pad(rows, ((0, 0), (0, row_pad), (0, 0)))


def rotate(cos_a, sin_a, cos_b, sin_b):
    return cos_a * cos_b - sin_a * sin_b, cos_a * sin_b + sin_a * cos_b


def build_base(ph_ref, base_ref, slot, wave_pad, scale_row):
    row = lax.broadcasted_iota(jnp.int32, (8, wave_pad), 0)
    cos_v = jnp.broadcast_to(ph_ref[slot, scale_row : scale_row + 1, :wave_pad], (8, wave_pad))
    sin_v = jnp.zeros((8, wave_pad), jnp.float32)
    for bit in range(3):
        on = ((row >> bit) & 1) == 1
        cos_b = jnp.where(on, ph_ref[slot, bit : bit + 1, :wave_pad], 1.0)
        sin_b = jnp.where(on, ph_ref[slot, bit : bit + 1, wave_pad:], 0.0)
        cos_v, sin_v = rotate(cos_v, sin_v, cos_b, sin_b)
    base_ref[0:8, :wave_pad] = cos_v
    base_ref[0:8, wave_pad:] = sin_v
    size, bit = 8, 3
    while size < KB:
        cos_b = ph_ref[slot, bit : bit + 1, :wave_pad]
        sin_b = ph_ref[slot, bit : bit + 1, wave_pad:]
        for start in range(0, size, 32):
            stop = min(start + 32, size)
            cos_v, sin_v = rotate(
                base_ref[start:stop, :wave_pad], base_ref[start:stop, wave_pad:], cos_b, sin_b
            )
            base_ref[size + start : size + stop, :wave_pad] = cos_v
            base_ref[size + start : size + stop, wave_pad:] = sin_v
        size, bit = size * 2, bit + 1


def table_block(ph_ref, base_ref, table_ref, slot, block, wave_pad):
    turn = ph_ref[slot, pl.ds(8 + block, 1), :]
    cos_b, sin_b = turn[:, :wave_pad], turn[:, wave_pad:]
    for start in range(0, KB, 32):
        stop = start + 32
        cos_v, sin_v = rotate(
            base_ref[start:stop, :wave_pad], base_ref[start:stop, wave_pad:], cos_b, sin_b
        )
        table_ref[start:stop, :wave_pad] = cos_v.astype(jnp.bfloat16)
        table_ref[start:stop, wave_pad:] = sin_v.astype(jnp.bfloat16)


def forward_kernel(
    wave_count, wave_pad, scale_row, first, groups, rest, len_ref, ph_ref, *refs
):
    if rest:
        grid_ref, grid_rest_ref, out_ref, base_ref, table_ref, wide_ref, acc_ref, rows_ref, wide_rest_ref, rest_ref = refs
        rest_cols = grid_rest_ref.shape[0]
        per_row = LANES // rest
        rest_rows = rest_ref.shape[0] // (2 * wave_count)
    else:
        grid_ref, out_ref, base_ref, table_ref, wide_ref, acc_ref, rows_ref = refs
        rest_cols = 0
    group = pl.program_id(0)
    segment = grid_ref.shape[2]
    owners, _, wave_dev = out_ref.shape[:3]

    def store_rows(source):
        for part in range(2):
            rows = source[part * wave_count * GROUP : (part + 1) * wave_count * GROUP, :]
            out_ref[:, part] = rows.reshape(owners, wave_dev, GROUP, LANES).astype(jnp.bfloat16)

    def run_group():
        for lane in range(segment // LANES):
            piece = grid_ref[:, :, lane * LANES : (lane + 1) * LANES].astype(jnp.float32)
            wide_ref[lane] = piece.reshape(LANES * GROUP, LANES)
            if rest:
                piece = grid_rest_ref[:, :, lane * LANES : (lane + 1) * LANES].astype(jnp.float32)
                wide_rest_ref[lane] = piece.reshape(rest_cols * GROUP, LANES)

        def per_slot(slot, carry):
            length = len_ref[(first + group) * GROUP + slot]
            build_base(ph_ref, base_ref, slot, wave_pad, scale_row)
            acc_ref[...] = jnp.zeros_like(acc_ref)

            def per_block(block, inner):
                table_block(ph_ref, base_ref, table_ref, slot, block, wave_pad)
                pieces = []
                for part in range(KB // LANES):
                    lane_block = block * (KB // LANES) + part
                    values = wide_ref[lane_block, pl.ds(slot, LANES, stride=GROUP), :]
                    if rest:
                        extra = wide_rest_ref[lane_block, pl.ds(slot, rest_cols, stride=GROUP), :]
                        values = jnp.concatenate([values, extra], axis=0)
                    at = lane_block * LANES + lax.broadcasted_iota(jnp.int32, values.shape, 1)
                    pieces.append(jnp.where(at < length, values, 0.0).astype(jnp.bfloat16))
                acc_ref[...] += jnp.dot(
                    jnp.concatenate(pieces, axis=1), table_ref[...], preferred_element_type=jnp.float32
                )
                return inner

            lax.fori_loop(0, (length + KB - 1) // KB, per_block, 0)
            for part in range(2):
                lanes = slice(part * wave_pad, (part + 1) * wave_pad)
                turned = acc_ref[:LANES, lanes].T
                rows_ref[pl.ds(part * wave_count * GROUP + slot, wave_count, stride=GROUP), :] = (
                    turned[:wave_count]
                )
                if rest:
                    cycle = (first + group) * GROUP + slot
                    turned = acc_ref[LANES:, lanes].T[:wave_count]
                    fill = jnp.zeros((wave_count, LANES - rest_cols), jnp.float32)
                    turned = jnp.concatenate([turned, fill], axis=1)
                    keep = lax.broadcasted_iota(jnp.int32, turned.shape, 1) < rest
                    turned = jnp.where(keep, turned, 0.0)
                    turned = pltpu.roll(turned, lax.rem(cycle, per_row) * rest, 1)
                    at = pl.ds(part * wave_count * rest_rows + cycle // per_row, wave_count, stride=rest_rows)
                    rest_ref[at, :] += turned
            return carry

        lax.fori_loop(0, GROUP, per_slot, 0)
        store_rows(rows_ref)

    if rest:

        @pl.when(group == 0)
        def _():
            rest_ref[...] = jnp.zeros_like(rest_ref)

        pl.when(group < groups)(run_group)

        @pl.when(group == groups)
        def _():
            store_rows(rest_ref)
    else:
        run_group()


def forward_dft(grid, lengths, phasors, owners, wave_count, wave_pad, scale_row, chunk, span):
    index, rest, rest_cols, rest_index = chunk
    _, _, segment = grid.shape
    first, groups = span[0], span[1] - span[0]
    wide_lanes = round_up(segment, KB) // LANES
    wave_dev = wave_count // owners
    rows = (groups + (1 if rest else 0)) * GROUP
    last = span[1] - 1
    in_specs = [
        pl.BlockSpec((GROUP,) + phasors.shape[1:], lambda g, n: (jnp.minimum(first + g, last), 0, 0)),
        pl.BlockSpec((LANES, GROUP, segment), lambda g, n: (index, jnp.minimum(first + g, last), 0)),
    ]
    operands = [lengths, phasors, grid]
    scratch = [
        pltpu.VMEM((KB, 2 * wave_pad), jnp.float32),
        pltpu.VMEM((KB, 2 * wave_pad), jnp.bfloat16),
        pltpu.VMEM((wide_lanes, LANES * GROUP, LANES), jnp.float32),
        pltpu.VMEM((LANES + rest_cols, 2 * wave_pad), jnp.float32),
        pltpu.VMEM((2 * wave_count * GROUP, LANES), jnp.float32),
    ]
    if rest:
        in_specs.append(
            pl.BlockSpec((rest_cols, GROUP, segment), lambda g, n: (rest_index, jnp.minimum(first + g, last), 0))
        )
        operands.append(grid)
        scratch += [
            pltpu.VMEM((wide_lanes, rest_cols * GROUP, LANES), jnp.float32),
            pltpu.VMEM((2 * wave_count * GROUP, LANES), jnp.float32),
        ]
    return pl.pallas_call(
        functools.partial(forward_kernel, wave_count, wave_pad, scale_row, first, groups, rest),
        out_shape=jax.ShapeDtypeStruct((owners, 2, wave_dev, rows, LANES), jnp.bfloat16),
        grid_spec=pltpu.PrefetchScalarGridSpec(
            num_scalar_prefetch=1,
            grid=(rows // GROUP,),
            in_specs=in_specs,
            out_specs=pl.BlockSpec((owners, 2, wave_dev, GROUP, LANES), lambda g, n: (0, 0, 0, g, 0)),
            scratch_shapes=scratch,
        ),
        compiler_params=pltpu.CompilerParams(
            dimension_semantics=("arbitrary",), vmem_limit_bytes=56 * 1024 * 1024
        ),
        cost_estimate=pl.CostEstimate(
            flops=2 * LANES * groups * GROUP * segment * wave_pad,
            bytes_accessed=2 * LANES * groups * GROUP * (segment + 2 * wave_count),
            transcendentals=0,
        ),
        name="forward_dft",
    )(*operands)


def adjoint_kernel(wave_count, wave_pad, scale_row, first, rest, aliased, len_ref, ph_ref, *refs):
    refs = list(refs)
    back_ref = refs.pop(0)
    back_rest_ref = refs.pop(0) if rest else None
    del refs[:aliased]
    out_ref = refs.pop(0)
    out_rest_ref = refs.pop(0) if rest else None
    base_ref, table_ref, lhs_ref, rows_ref, wide_ref = refs[:5]
    if rest:
        wide_rest_ref, rest_ref = refs[5:]
        rest_cols = out_rest_ref.shape[0]
        per_row = LANES // rest
    group = pl.program_id(0)
    segment = out_ref.shape[2]
    lane_count = wide_ref.shape[0]
    per_kb = KB // LANES
    span = wave_count * GROUP
    for part in range(2):
        rows_ref[part * span : (part + 1) * span, :] = (
            back_ref[:, part].astype(jnp.float32).reshape(span, LANES)
        )

    @pl.when(group == 0)
    def _():
        lhs_ref[...] = jnp.zeros_like(lhs_ref)
        if rest:
            for part in range(2):
                rest_ref[part * span : (part + 1) * span, :] = (
                    back_rest_ref[:, part].astype(jnp.float32).reshape(span, LANES)
                )

    def put(slot, lane_block, values):
        wide_ref[lane_block, pl.ds(slot, LANES, stride=GROUP), :] = values[:LANES]
        if rest:
            wide_rest_ref[lane_block, pl.ds(slot, rest_cols, stride=GROUP), :] = values[LANES:]

    def per_slot(slot, carry):
        length = len_ref[(first + group) * GROUP + slot]
        build_base(ph_ref, base_ref, slot, wave_pad, scale_row)
        for part in range(2):
            lanes = slice(part * wave_pad, part * wave_pad + wave_count)
            turned = rows_ref[pl.ds(part * span + slot, wave_count, stride=GROUP), :].T
            lhs_ref[:LANES, lanes] = turned.astype(jnp.bfloat16)
            if rest:
                cycle = (first + group) * GROUP + slot
                rows = rest_ref[pl.ds(part * span + cycle // per_row, wave_count, stride=GROUP), :]
                rows = pltpu.roll(rows, LANES - lax.rem(cycle, per_row) * rest, 1)
                lhs_ref[LANES:, lanes] = rows[:, :rest_cols].T.astype(jnp.bfloat16)
        used = (length + KB - 1) // KB

        def per_block(block, inner):
            table_block(ph_ref, base_ref, table_ref, slot, block, wave_pad)
            values = lax.dot_general(
                lhs_ref[...], table_ref[...], (((1,), (1,)), ((), ())), preferred_element_type=jnp.float32
            )
            for part in range(per_kb):
                lane_block = block * per_kb + part
                piece = values[:, part * LANES : (part + 1) * LANES]
                at = lane_block * LANES + lax.broadcasted_iota(jnp.int32, piece.shape, 1)
                put(slot, lane_block, jnp.where(at < length, piece, 0.0))
            return inner

        def fill(lane_block, inner):
            put(slot, lane_block, jnp.zeros((lhs_ref.shape[0], LANES), jnp.float32))
            return inner

        lax.fori_loop(0, used, per_block, 0)
        lax.fori_loop(used * per_kb, lane_count, fill, 0)
        return carry

    lax.fori_loop(0, GROUP, per_slot, 0)
    for lane in range(segment // LANES):
        lanes = slice(lane * LANES, (lane + 1) * LANES)
        out_ref[:, :, lanes] = wide_ref[lane].reshape(LANES, GROUP, LANES).astype(jnp.bfloat16)
        if rest:
            values = wide_rest_ref[lane].reshape(rest_cols, GROUP, LANES)
            out_rest_ref[:, :, lanes] = values.astype(jnp.bfloat16)


def adjoint_dft(back, back_rest, fields, lengths, phasors, out_shape, wave_count, wave_pad, scale_row, chunk, span):
    index, rest, rest_cols, _ = chunk
    _, cycle_dev, segment = out_shape
    owners, _, wave_dev, _, _ = back.shape
    first, groups = span[0], span[1] - span[0]
    wide_lanes = round_up(segment, KB) // LANES
    aliased = len(fields)
    block = (owners, 2, wave_dev, GROUP, LANES)
    in_specs = [
        pl.BlockSpec((GROUP,) + phasors.shape[1:], lambda g, n: (first + g, 0, 0)),
        pl.BlockSpec(block, lambda g, n: (0, 0, 0, g, 0)),
    ]
    operands = [lengths, phasors, back]
    out_specs = [pl.BlockSpec((LANES, GROUP, segment), lambda g, n: (index, first + g, 0))]
    out_shapes = [jax.ShapeDtypeStruct(out_shape, jnp.bfloat16)]
    scratch = [
        pltpu.VMEM((KB, 2 * wave_pad), jnp.float32),
        pltpu.VMEM((KB, 2 * wave_pad), jnp.bfloat16),
        pltpu.VMEM((LANES + rest_cols, 2 * wave_pad), jnp.bfloat16),
        pltpu.VMEM((2 * wave_count * GROUP, LANES), jnp.float32),
        pltpu.VMEM((wide_lanes, LANES * GROUP, LANES), jnp.float32),
    ]
    if rest:
        rest_block = back_rest.shape[3] // GROUP - 1
        in_specs.append(pl.BlockSpec(block, lambda g, n: (0, 0, 0, rest_block, 0)))
        operands.append(back_rest)
        out_specs.append(pl.BlockSpec((rest_cols, GROUP, segment), lambda g, n: (0, first + g, 0)))
        out_shapes.append(jax.ShapeDtypeStruct((rest_cols, cycle_dev, segment), jnp.bfloat16))
        scratch += [
            pltpu.VMEM((wide_lanes, rest_cols * GROUP, LANES), jnp.float32),
            pltpu.VMEM((2 * wave_count * GROUP, LANES), jnp.float32),
        ]
    aliases = {}
    for output, field in enumerate(fields):
        aliases[len(operands)] = output
        in_specs.append(pl.BlockSpec(memory_space=pl.ANY))
        operands.append(field)
    return pl.pallas_call(
        functools.partial(adjoint_kernel, wave_count, wave_pad, scale_row, first, rest, aliased),
        out_shape=out_shapes,
        grid_spec=pltpu.PrefetchScalarGridSpec(
            num_scalar_prefetch=1, grid=(groups,), in_specs=in_specs, out_specs=out_specs, scratch_shapes=scratch
        ),
        input_output_aliases=aliases,
        compiler_params=pltpu.CompilerParams(
            dimension_semantics=("arbitrary",), vmem_limit_bytes=60 * 1024 * 1024
        ),
        cost_estimate=pl.CostEstimate(
            flops=2 * LANES * groups * GROUP * segment * wave_pad,
            bytes_accessed=2 * LANES * groups * GROUP * (segment + 2 * wave_count),
            transcendentals=0,
        ),
        name="adjoint_dft",
    )(*operands)


def column_chunks(col_count):
    whole = col_count // LANES
    rest = col_count - whole * LANES
    chunks = [(index, 0, 0, 0) for index in range(whole)]
    if rest:
        width = 8
        while width < rest:
            width *= 2
        chunks[-1] = (whole - 1, rest, width, whole * LANES // width)
    return chunks


def device_program(grid, cycle_ids, cycle_len, wave_ids, legendre, target, step_w, chan_w):
    _, batch_size, chan_count, cycle_dev, segment = grid.shape
    wave_count = wave_ids.shape[0]
    wave_dev, degree_count, _ = legendre.shape
    owners = wave_count // wave_dev
    col_count = batch_size * chan_count
    wave_pad = round_up(wave_count, LANES)
    block_count = pl.cdiv(segment, KB)
    scale_row = 8 + block_count
    lat_index = lax.axis_index("lat")
    my_cycles = lax.dynamic_slice_in_dim(cycle_ids, lat_index * cycle_dev, cycle_dev)
    lengths = jnp.take(cycle_len, my_cycles)
    phasors = phasor_rows(lengths, wave_ids, block_count, wave_pad)
    group_pad = round_up(cycle_dev, GROUP) - cycle_dev
    if group_pad:
        lengths = jnp.pad(lengths, (0, group_pad))
        phasors = jnp.pad(phasors, ((0, group_pad), (0, 0), (0, 0)))
    grid3 = grid.reshape(col_count, cycle_dev, segment)
    my_waves = lax.dynamic_slice_in_dim(wave_ids, lat_index * wave_dev, wave_dev)
    degree = jnp.arange(degree_count, dtype=jnp.int32)
    kept = (degree[None, :] >= my_waves[:, None]).astype(jnp.float32)[:, :, None, None]
    factor = jnp.where(my_waves == 0, 1.0, 2.0).astype(jnp.float32)
    weight_cols = jnp.broadcast_to(step_w[0] * chan_w[None, :], (batch_size, chan_count)).reshape(
        col_count
    )
    target3 = target.reshape(col_count, 2, wave_dev, degree_count)

    def exchange(values):
        shape = values.shape
        flat = values.reshape((owners * 2 * wave_dev,) + shape[3:])
        return lax.all_to_all(flat, "lat", split_axis=0, concat_axis=0, tiled=True).reshape(shape)

    chunks = column_chunks(col_count)
    groups = pl.cdiv(cycle_dev, GROUP)
    last = len(chunks) - 1
    head, tail = max(1, groups // 5), max(1, 2 * groups // 5)
    spans_out = [[(0, groups)] for _ in chunks]
    spans_back = [[(0, groups)] for _ in chunks]
    if groups > 1:
        spans_out[0] = [(0, head), (head, groups)]
        spans_back[last] = [(0, groups - tail), (groups - tail, groups)]
    sent = []
    for number, chunk in enumerate(chunks):
        parts = []
        for span in spans_out[number]:
            rides = chunk if span[1] == groups else (chunk[0], 0, 0, 0)
            part = forward_dft(
                grid3, lengths, phasors, owners, wave_count, wave_pad, scale_row, rides, span
            )
            part, lengths, legendre, target3 = lax.optimization_barrier((part, lengths, legendre, target3))
            parts.append(part)
        sent.append(parts)
    legendre_cols = jnp.take(legendre, cycle_ids, axis=2).reshape(
        wave_dev, degree_count, owners, cycle_dev
    )

    def owner_pass(gathered, start, cols):
        coeffs = jnp.einsum(
            "sndp,dtspc->sntc", legendre_cols, gathered, preferred_element_type=jnp.float32
        )
        coeffs = coeffs * kept
        goal = jnp.transpose(target3[start : start + cols], (2, 3, 1, 0))
        weight = factor[:, None, None, None] * weight_cols[None, None, None, start : start + cols]
        misfit = (coeffs - goal) * kept
        value = jnp.sum(weight * misfit * misfit)
        grad_coeff = (2.0 * weight * misfit).astype(jnp.bfloat16)
        back = jnp.einsum(
            "sndp,sntc->dtspc", legendre_cols, grad_coeff, preferred_element_type=jnp.float32
        ).astype(jnp.bfloat16)
        return jnp.transpose(coeffs, (3, 2, 0, 1)), value, back

    partial_value = jnp.float32(0.0)
    coeff_parts, backs = [], []
    for number, chunk in enumerate(chunks):
        index, rest = chunk[:2]
        gathered = [exchange(part) for part in sent[number]]
        gathered = gathered[0] if len(gathered) == 1 else jnp.concatenate(gathered, axis=3)
        coeff_part, value, back = owner_pass(gathered[:, :, :, :cycle_dev], index * LANES, LANES)
        coeff_parts.append(coeff_part)
        partial_value = partial_value + value
        row_pad = groups * GROUP - cycle_dev
        if row_pad:
            back = jnp.pad(back, ((0, 0),) * 3 + ((0, row_pad), (0, 0)))
        pieces = [back[:, :, :, span[0] * GROUP : span[1] * GROUP] for span in spans_back[number]]
        if rest:
            per_row = LANES // rest
            lead = gathered.shape[:3]
            packed = gathered[:, :, :, groups * GROUP :, : per_row * rest]
            unpacked = packed.reshape(lead + (GROUP * per_row, rest))[:, :, :, :cycle_dev]
            coeff_part, value, back_rest = owner_pass(unpacked, col_count - rest, rest)
            coeff_parts.append(coeff_part)
            partial_value = partial_value + value
            back_rest = jnp.pad(back_rest, ((0, 0),) * 3 + ((0, GROUP * per_row - cycle_dev), (0, 0)))
            back_rest = back_rest.reshape(lead + (GROUP, per_row * rest))
            back_rest = jnp.pad(back_rest, ((0, 0),) * 4 + ((0, LANES - per_row * rest),))
            pieces[0] = jnp.concatenate([pieces[0], back_rest], axis=3)
        backs.append(pieces)
    coeff_out = jnp.concatenate(coeff_parts, axis=0)
    coeff_out = coeff_out.reshape(1, batch_size, chan_count, 2, wave_dev, degree_count)
    fields, loss_sum = [], None
    steps = [
        (chunk, part, span, backs[number][part])
        for number, chunk in enumerate(chunks)
        for part, span in enumerate(spans_back[number])
    ]
    returned_rest = None
    for number, (chunk, part, span, back) in enumerate(steps):
        if loss_sum is not None and number == len(steps) - 1:
            back, loss_sum = lax.optimization_barrier((back, loss_sum))
        returned = exchange(back)
        returned_rest = returned if part == 0 else returned_rest
        fields = list(
            adjoint_dft(
                returned, returned_rest, fields, lengths, phasors, grid3.shape, wave_count, wave_pad,
                scale_row, chunk, span,
            )
        )
        if loss_sum is None:
            fields[0], partial_value = lax.optimization_barrier((fields[0], partial_value))
            loss_sum = lax.psum(partial_value, ("lat", "fld"))
    field = fields[0]
    if chunks[last][1]:
        rest = chunks[last][1]
        field = lax.dynamic_update_slice(field, fields[1][:rest], (col_count - rest, 0, 0))
    term_count = STEPS * col_count * wave_count * (wave_count + 1) // 2
    loss = loss_sum / jnp.float32(term_count)
    return (
        coeff_out,
        loss,
        field.reshape(1, batch_size, chan_count, cycle_dev, segment),
    )


def solution(mesh):
    return jax.shard_map(
        device_program,
        mesh=mesh,
        in_specs=(
            P("fld", None, None, "lat", None),
            P(),
            P(),
            P(),
            P("lat", None, None),
            P("fld", None, None, None, "lat", None),
            P("fld"),
            P(),
        ),
        out_specs=(P("fld", None, None, None, "lat", None), P(), P("fld", None, None, "lat", None)),
        check_vma=False,
    )
```

```python
import functools
import math

import jax
import jax.numpy as jnp
from jax import lax
from jax.experimental import pallas as pl
from jax.experimental.pallas import tpu as pltpu
from jax.sharding import PartitionSpec as P


STEPS = 2
KB = 256
GROUP = 8
LANES = 128
SPLIT = 3


def round_up(value, unit):
    return (value + unit - 1) // unit * unit


def phasor_rows(lengths, wave_ids, block_count, wave_pad):
    exponents = [1 << bit for bit in range(8)] + [KB * block for block in range(block_count)]
    exponents = jnp.asarray(exponents, dtype=jnp.int32)
    length = lengths[:, None, None]
    length_f = length.astype(jnp.float32)
    product = (exponents[None, :, None] * wave_ids[None, None, :]).astype(jnp.float32)
    inverse = 1.0 / length_f
    phase = product - jnp.floor(product * inverse) * length_f
    phase = jnp.where(phase < 0.0, phase + length_f, phase)
    phase = jnp.where(phase >= length_f, phase - length_f, phase)
    turn = phase * inverse
    quarter = jnp.floor(turn * 4.0 + 0.5)
    x = (turn - 0.25 * quarter) * jnp.float32(2.0 * math.pi)
    x2 = x * x
    sin_x = x * (1.0 + x2 * (-1.0 / 6 + x2 * (1.0 / 120 + x2 * (-1.0 / 5040 + x2 * (1.0 / 362880)))))
    cos_x = 1.0 + x2 * (
        -0.5 + x2 * (1.0 / 24 + x2 * (-1.0 / 720 + x2 * (1.0 / 40320 + x2 * (-1.0 / 3628800))))
    )
    odd = (quarter == 1.0) | (quarter == 3.0)
    cos_t = jnp.where(odd, sin_x, cos_x)
    cos_t = jnp.where((quarter == 1.0) | (quarter == 2.0), -cos_t, cos_t)
    sin_t = jnp.where(odd, cos_x, sin_x)
    sin_t = jnp.where((quarter == 2.0) | (quarter == 3.0), -sin_t, sin_t)
    scale = jnp.where(2 * wave_ids[None, None, :] < length, lax.rsqrt(length_f), jnp.float32(0.0))
    lane_pad = ((0, 0), (0, 0), (0, wave_pad - wave_ids.shape[0]))
    cos_t = jnp.concatenate([cos_t, scale], axis=1)
    sin_t = jnp.concatenate([-sin_t, jnp.zeros_like(scale)], axis=1)
    rows = jnp.concatenate([jnp.pad(cos_t, lane_pad), jnp.pad(sin_t, lane_pad)], axis=2)
    row_pad = round_up(rows.shape[1], 8) - rows.shape[1]
    return jnp.pad(rows, ((0, 0), (0, row_pad), (0, 0)))


def rotate(cos_a, sin_a, cos_b, sin_b):
    return cos_a * cos_b - sin_a * sin_b, cos_a * sin_b + sin_a * cos_b


def build_base(ph_ref, base_ref, slot, wave_pad, scale_row):
    row = lax.broadcasted_iota(jnp.int32, (8, wave_pad), 0)
    cos_v = jnp.broadcast_to(ph_ref[slot, scale_row : scale_row + 1, :wave_pad], (8, wave_pad))
    sin_v = jnp.zeros((8, wave_pad), jnp.float32)
    for bit in range(3):
        on = ((row >> bit) & 1) == 1
        cos_b = jnp.where(on, ph_ref[slot, bit : bit + 1, :wave_pad], 1.0)
        sin_b = jnp.where(on, ph_ref[slot, bit : bit + 1, wave_pad:], 0.0)
        cos_v, sin_v = rotate(cos_v, sin_v, cos_b, sin_b)
    base_ref[0:8, :wave_pad] = cos_v
    base_ref[0:8, wave_pad:] = sin_v
    size, bit = 8, 3
    while size < KB:
        cos_b = ph_ref[slot, bit : bit + 1, :wave_pad]
        sin_b = ph_ref[slot, bit : bit + 1, wave_pad:]
        for start in range(0, size, 32):
            stop = min(start + 32, size)
            cos_v, sin_v = rotate(
                base_ref[start:stop, :wave_pad], base_ref[start:stop, wave_pad:], cos_b, sin_b
            )
            base_ref[size + start : size + stop, :wave_pad] = cos_v
            base_ref[size + start : size + stop, wave_pad:] = sin_v
        size, bit = size * 2, bit + 1


def table_block(ph_ref, base_ref, table_ref, slot, block, wave_pad):
    turn = ph_ref[slot, pl.ds(8 + block, 1), :]
    cos_b, sin_b = turn[:, :wave_pad], turn[:, wave_pad:]
    for start in range(0, KB, 32):
        stop = start + 32
        cos_v, sin_v = rotate(
            base_ref[start:stop, :wave_pad], base_ref[start:stop, wave_pad:], cos_b, sin_b
        )
        table_ref[start:stop, :wave_pad] = cos_v.astype(jnp.bfloat16)
        table_ref[start:stop, wave_pad:] = sin_v.astype(jnp.bfloat16)


def forward_kernel(
    wave_count, wave_pad, scale_row, first, groups, rest, len_ref, ph_ref, *refs
):
    if rest:
        grid_ref, grid_rest_ref, out_ref, base_ref, table_ref, wide_ref, acc_ref, rows_ref, wide_rest_ref, rest_ref = refs
        rest_cols = grid_rest_ref.shape[0]
        per_row = LANES // rest
        rest_rows = rest_ref.shape[0] // (2 * wave_count)
    else:
        grid_ref, out_ref, base_ref, table_ref, wide_ref, acc_ref, rows_ref = refs
        rest_cols = 0
    group = pl.program_id(0)
    segment = grid_ref.shape[2]
    owners, _, wave_dev = out_ref.shape[:3]

    def store_rows(source):
        for part in range(2):
            rows = source[part * wave_count * GROUP : (part + 1) * wave_count * GROUP, :]
            out_ref[:, part] = rows.reshape(owners, wave_dev, GROUP, LANES).astype(jnp.bfloat16)

    def run_group():
        for lane in range(segment // LANES):
            piece = grid_ref[:, :, lane * LANES : (lane + 1) * LANES].astype(jnp.float32)
            wide_ref[lane] = piece.reshape(LANES * GROUP, LANES)
            if rest:
                piece = grid_rest_ref[:, :, lane * LANES : (lane + 1) * LANES].astype(jnp.float32)
                wide_rest_ref[lane] = piece.reshape(rest_cols * GROUP, LANES)

        def per_slot(slot, carry):
            length = len_ref[(first + group) * GROUP + slot]
            build_base(ph_ref, base_ref, slot, wave_pad, scale_row)
            acc_ref[...] = jnp.zeros_like(acc_ref)

            def per_block(block, inner):
                table_block(ph_ref, base_ref, table_ref, slot, block, wave_pad)
                pieces = []
                for part in range(KB // LANES):
                    lane_block = block * (KB // LANES) + part
                    values = wide_ref[lane_block, pl.ds(slot, LANES, stride=GROUP), :]
                    if rest:
                        extra = wide_rest_ref[lane_block, pl.ds(slot, rest_cols, stride=GROUP), :]
                        values = jnp.concatenate([values, extra], axis=0)
                    at = lane_block * LANES + lax.broadcasted_iota(jnp.int32, values.shape, 1)
                    pieces.append(jnp.where(at < length, values, 0.0).astype(jnp.bfloat16))
                acc_ref[...] += jnp.dot(
                    jnp.concatenate(pieces, axis=1), table_ref[...], preferred_element_type=jnp.float32
                )
                return inner

            lax.fori_loop(0, (length + KB - 1) // KB, per_block, 0)
            for part in range(2):
                lanes = slice(part * wave_pad, (part + 1) * wave_pad)
                turned = acc_ref[:LANES, lanes].T
                rows_ref[pl.ds(part * wave_count * GROUP + slot, wave_count, stride=GROUP), :] = (
                    turned[:wave_count]
                )
                if rest:
                    cycle = (first + group) * GROUP + slot
                    turned = acc_ref[LANES:, lanes].T[:wave_count]
                    fill = jnp.zeros((wave_count, LANES - rest_cols), jnp.float32)
                    turned = jnp.concatenate([turned, fill], axis=1)
                    keep = lax.broadcasted_iota(jnp.int32, turned.shape, 1) < rest
                    turned = jnp.where(keep, turned, 0.0)
                    turned = pltpu.roll(turned, lax.rem(cycle, per_row) * rest, 1)
                    at = pl.ds(part * wave_count * rest_rows + cycle // per_row, wave_count, stride=rest_rows)
                    rest_ref[at, :] += turned
            return carry

        lax.fori_loop(0, GROUP, per_slot, 0)
        store_rows(rows_ref)

    if rest:

        @pl.when(group == 0)
        def _():
            rest_ref[...] = jnp.zeros_like(rest_ref)

        pl.when(group < groups)(run_group)

        @pl.when(group == groups)
        def _():
            store_rows(rest_ref)
    else:
        run_group()


def forward_dft(grid, lengths, phasors, owners, wave_count, wave_pad, scale_row, chunk, span):
    index, rest, rest_cols, rest_index = chunk
    _, _, segment = grid.shape
    first, groups = span[0], span[1] - span[0]
    wide_lanes = round_up(segment, KB) // LANES
    wave_dev = wave_count // owners
    rows = (groups + (1 if rest else 0)) * GROUP
    last = span[1] - 1
    in_specs = [
        pl.BlockSpec((GROUP,) + phasors.shape[1:], lambda g, n: (jnp.minimum(first + g, last), 0, 0)),
        pl.BlockSpec((LANES, GROUP, segment), lambda g, n: (index, jnp.minimum(first + g, last), 0)),
    ]
    operands = [lengths, phasors, grid]
    scratch = [
        pltpu.VMEM((KB, 2 * wave_pad), jnp.float32),
        pltpu.VMEM((KB, 2 * wave_pad), jnp.bfloat16),
        pltpu.VMEM((wide_lanes, LANES * GROUP, LANES), jnp.float32),
        pltpu.VMEM((LANES + rest_cols, 2 * wave_pad), jnp.float32),
        pltpu.VMEM((2 * wave_count * GROUP, LANES), jnp.float32),
    ]
    if rest:
        in_specs.append(
            pl.BlockSpec((rest_cols, GROUP, segment), lambda g, n: (rest_index, jnp.minimum(first + g, last), 0))
        )
        operands.append(grid)
        scratch += [
            pltpu.VMEM((wide_lanes, rest_cols * GROUP, LANES), jnp.float32),
            pltpu.VMEM((2 * wave_count * GROUP, LANES), jnp.float32),
        ]
    return pl.pallas_call(
        functools.partial(forward_kernel, wave_count, wave_pad, scale_row, first, groups, rest),
        out_shape=jax.ShapeDtypeStruct((owners, 2, wave_dev, rows, LANES), jnp.bfloat16),
        grid_spec=pltpu.PrefetchScalarGridSpec(
            num_scalar_prefetch=1,
            grid=(rows // GROUP,),
            in_specs=in_specs,
            out_specs=pl.BlockSpec((owners, 2, wave_dev, GROUP, LANES), lambda g, n: (0, 0, 0, g, 0)),
            scratch_shapes=scratch,
        ),
        compiler_params=pltpu.CompilerParams(
            dimension_semantics=("arbitrary",), vmem_limit_bytes=56 * 1024 * 1024
        ),
        cost_estimate=pl.CostEstimate(
            flops=2 * LANES * groups * GROUP * segment * wave_pad,
            bytes_accessed=2 * LANES * groups * GROUP * (segment + 2 * wave_count),
            transcendentals=0,
        ),
        name="forward_dft",
    )(*operands)


def adjoint_kernel(wave_count, wave_pad, scale_row, first, rest, aliased, len_ref, ph_ref, *refs):
    refs = list(refs)
    back_ref = refs.pop(0)
    back_rest_ref = refs.pop(0) if rest else None
    del refs[:aliased]
    out_ref = refs.pop(0)
    out_rest_ref = refs.pop(0) if rest else None
    base_ref, table_ref, lhs_ref, rows_ref, wide_ref = refs[:5]
    if rest:
        wide_rest_ref, rest_ref = refs[5:]
        rest_cols = out_rest_ref.shape[0]
        per_row = LANES // rest
    group = pl.program_id(0)
    segment = out_ref.shape[2]
    lane_count = wide_ref.shape[0]
    per_kb = KB // LANES
    span = wave_count * GROUP
    for part in range(2):
        rows_ref[part * span : (part + 1) * span, :] = (
            back_ref[:, part].astype(jnp.float32).reshape(span, LANES)
        )

    @pl.when(group == 0)
    def _():
        lhs_ref[...] = jnp.zeros_like(lhs_ref)
        if rest:
            for part in range(2):
                rest_ref[part * span : (part + 1) * span, :] = (
                    back_rest_ref[:, part].astype(jnp.float32).reshape(span, LANES)
                )

    def put(slot, lane_block, values):
        wide_ref[lane_block, pl.ds(slot, LANES, stride=GROUP), :] = values[:LANES]
        if rest:
            wide_rest_ref[lane_block, pl.ds(slot, rest_cols, stride=GROUP), :] = values[LANES:]

    def per_slot(slot, carry):
        length = len_ref[(first + group) * GROUP + slot]
        build_base(ph_ref, base_ref, slot, wave_pad, scale_row)
        for part in range(2):
            lanes = slice(part * wave_pad, part * wave_pad + wave_count)
            turned = rows_ref[pl.ds(part * span + slot, wave_count, stride=GROUP), :].T
            lhs_ref[:LANES, lanes] = turned.astype(jnp.bfloat16)
            if rest:
                cycle = (first + group) * GROUP + slot
                rows = rest_ref[pl.ds(part * span + cycle // per_row, wave_count, stride=GROUP), :]
                rows = pltpu.roll(rows, LANES - lax.rem(cycle, per_row) * rest, 1)
                lhs_ref[LANES:, lanes] = rows[:, :rest_cols].T.astype(jnp.bfloat16)
        used = (length + KB - 1) // KB

        def per_block(block, inner):
            table_block(ph_ref, base_ref, table_ref, slot, block, wave_pad)
            values = lax.dot_general(
                lhs_ref[...], table_ref[...], (((1,), (1,)), ((), ())), preferred_element_type=jnp.float32
            )
            for part in range(per_kb):
                lane_block = block * per_kb + part
                piece = values[:, part * LANES : (part + 1) * LANES]
                at = lane_block * LANES + lax.broadcasted_iota(jnp.int32, piece.shape, 1)
                put(slot, lane_block, jnp.where(at < length, piece, 0.0))
            return inner

        def fill(lane_block, inner):
            put(slot, lane_block, jnp.zeros((lhs_ref.shape[0], LANES), jnp.float32))
            return inner

        lax.fori_loop(0, used, per_block, 0)
        lax.fori_loop(used * per_kb, lane_count, fill, 0)
        return carry

    lax.fori_loop(0, GROUP, per_slot, 0)
    for lane in range(segment // LANES):
        lanes = slice(lane * LANES, (lane + 1) * LANES)
        out_ref[:, :, lanes] = wide_ref[lane].reshape(LANES, GROUP, LANES).astype(jnp.bfloat16)
        if rest:
            values = wide_rest_ref[lane].reshape(rest_cols, GROUP, LANES)
            out_rest_ref[:, :, lanes] = values.astype(jnp.bfloat16)


def adjoint_dft(back, back_rest, fields, lengths, phasors, out_shape, wave_count, wave_pad, scale_row, chunk, span):
    index, rest, rest_cols, _ = chunk
    _, cycle_dev, segment = out_shape
    owners, _, wave_dev, _, _ = back.shape
    first, groups = span[0], span[1] - span[0]
    wide_lanes = round_up(segment, KB) // LANES
    aliased = len(fields)
    block = (owners, 2, wave_dev, GROUP, LANES)
    in_specs = [
        pl.BlockSpec((GROUP,) + phasors.shape[1:], lambda g, n: (first + g, 0, 0)),
        pl.BlockSpec(block, lambda g, n: (0, 0, 0, g, 0)),
    ]
    operands = [lengths, phasors, back]
    out_specs = [pl.BlockSpec((LANES, GROUP, segment), lambda g, n: (index, first + g, 0))]
    out_shapes = [jax.ShapeDtypeStruct(out_shape, jnp.bfloat16)]
    scratch = [
        pltpu.VMEM((KB, 2 * wave_pad), jnp.float32),
        pltpu.VMEM((KB, 2 * wave_pad), jnp.bfloat16),
        pltpu.VMEM((LANES + rest_cols, 2 * wave_pad), jnp.bfloat16),
        pltpu.VMEM((2 * wave_count * GROUP, LANES), jnp.float32),
        pltpu.VMEM((wide_lanes, LANES * GROUP, LANES), jnp.float32),
    ]
    if rest:
        rest_block = back_rest.shape[3] // GROUP - 1
        in_specs.append(pl.BlockSpec(block, lambda g, n: (0, 0, 0, rest_block, 0)))
        operands.append(back_rest)
        out_specs.append(pl.BlockSpec((rest_cols, GROUP, segment), lambda g, n: (0, first + g, 0)))
        out_shapes.append(jax.ShapeDtypeStruct((rest_cols, cycle_dev, segment), jnp.bfloat16))
        scratch += [
            pltpu.VMEM((wide_lanes, rest_cols * GROUP, LANES), jnp.float32),
            pltpu.VMEM((2 * wave_count * GROUP, LANES), jnp.float32),
        ]
    aliases = {}
    for output, field in enumerate(fields):
        aliases[len(operands)] = output
        in_specs.append(pl.BlockSpec(memory_space=pl.ANY))
        operands.append(field)
    return pl.pallas_call(
        functools.partial(adjoint_kernel, wave_count, wave_pad, scale_row, first, rest, aliased),
        out_shape=out_shapes,
        grid_spec=pltpu.PrefetchScalarGridSpec(
            num_scalar_prefetch=1, grid=(groups,), in_specs=in_specs, out_specs=out_specs, scratch_shapes=scratch
        ),
        input_output_aliases=aliases,
        compiler_params=pltpu.CompilerParams(
            dimension_semantics=("arbitrary",), vmem_limit_bytes=60 * 1024 * 1024
        ),
        cost_estimate=pl.CostEstimate(
            flops=2 * LANES * groups * GROUP * segment * wave_pad,
            bytes_accessed=2 * LANES * groups * GROUP * (segment + 2 * wave_count),
            transcendentals=0,
        ),
        name="adjoint_dft",
    )(*operands)


def split_terms(value):
    terms = []
    for _ in range(SPLIT):
        term = lax.reduce_precision(value, exponent_bits=8, mantissa_bits=7)
        terms.append(term.astype(jnp.bfloat16))
        value = value - term
    return terms


def place_terms(rows, terms, lane):
    at = [lax.broadcasted_iota(jnp.int32, rows.shape, axis) for axis in range(1, rows.ndim)]
    first = (at[0] == 0) & (at[1] == 0) & (at[2] == 0)
    for number, term in enumerate(terms):
        rows = jnp.where(first & (at[3] == lane + number), term, rows)
    return rows


def column_chunks(col_count):
    whole = col_count // LANES
    rest = col_count - whole * LANES
    chunks = [(index, 0, 0, 0) for index in range(whole)]
    if rest:
        width = 8
        while width < rest:
            width *= 2
        chunks[-1] = (whole - 1, rest, width, whole * LANES // width)
    return chunks


def device_program(grid, cycle_ids, cycle_len, wave_ids, legendre, target, step_w, chan_w):
    _, batch_size, chan_count, cycle_dev, segment = grid.shape
    wave_count = wave_ids.shape[0]
    wave_dev, degree_count, _ = legendre.shape
    owners = wave_count // wave_dev
    col_count = batch_size * chan_count
    wave_pad = round_up(wave_count, LANES)
    block_count = pl.cdiv(segment, KB)
    scale_row = 8 + block_count
    lat_index = lax.axis_index("lat")
    my_cycles = lax.dynamic_slice_in_dim(cycle_ids, lat_index * cycle_dev, cycle_dev)
    lengths = jnp.take(cycle_len, my_cycles)
    phasors = phasor_rows(lengths, wave_ids, block_count, wave_pad)
    group_pad = round_up(cycle_dev, GROUP) - cycle_dev
    if group_pad:
        lengths = jnp.pad(lengths, (0, group_pad))
        phasors = jnp.pad(phasors, ((0, group_pad), (0, 0), (0, 0)))
    grid3 = grid.reshape(col_count, cycle_dev, segment)
    my_waves = lax.dynamic_slice_in_dim(wave_ids, lat_index * wave_dev, wave_dev)
    degree = jnp.arange(degree_count, dtype=jnp.int32)
    kept = (degree[None, :] >= my_waves[:, None]).astype(jnp.float32)[:, :, None, None]
    factor = jnp.where(my_waves == 0, 1.0, 2.0).astype(jnp.float32)
    weight_cols = jnp.broadcast_to(step_w[0] * chan_w[None, :], (batch_size, chan_count)).reshape(
        col_count
    )
    target3 = target.reshape(col_count, 2, wave_dev, degree_count)

    def exchange(values):
        shape = values.shape
        flat = values.reshape((owners * 2 * wave_dev,) + shape[3:])
        return lax.all_to_all(flat, "lat", split_axis=0, concat_axis=0, tiled=True).reshape(shape)

    chunks = column_chunks(col_count)
    groups = pl.cdiv(cycle_dev, GROUP)
    last = len(chunks) - 1
    head = tail = max(1, 2 * groups // 5)
    spans_out = [[(0, groups)] for _ in chunks]
    spans_back = [[(0, groups)] for _ in chunks]
    if groups > 1:
        spans_out[0] = [(0, head), (head, groups)]
        spans_back[last] = [(0, groups - tail), (groups - tail, groups)]
    sent = []
    for number, chunk in enumerate(chunks):
        parts = []
        for span in spans_out[number]:
            rides = chunk if span[1] == groups else (chunk[0], 0, 0, 0)
            part = forward_dft(
                grid3, lengths, phasors, owners, wave_count, wave_pad, scale_row, rides, span
            )
            part, lengths, legendre, target3 = lax.optimization_barrier((part, lengths, legendre, target3))
            parts.append(part)
        sent.append(parts)
    legendre_cols = jnp.take(legendre, cycle_ids, axis=2).reshape(
        wave_dev, degree_count, owners, cycle_dev
    )

    def owner_pass(gathered, start, cols):
        coeffs = jnp.einsum(
            "sndp,dtspc->sntc", legendre_cols, gathered, preferred_element_type=jnp.float32
        )
        coeffs = coeffs * kept
        goal = jnp.transpose(target3[start : start + cols], (2, 3, 1, 0))
        weight = factor[:, None, None, None] * weight_cols[None, None, None, start : start + cols]
        misfit = (coeffs - goal) * kept
        value = jnp.sum(weight * misfit * misfit)
        grad_coeff = (2.0 * weight * misfit).astype(jnp.bfloat16)
        back = jnp.einsum(
            "sndp,sntc->dtspc", legendre_cols, grad_coeff, preferred_element_type=jnp.float32
        ).astype(jnp.bfloat16)
        return jnp.transpose(coeffs, (3, 2, 0, 1)), value, back

    partial_value = jnp.float32(0.0)
    loss_lane = None
    coeff_parts, backs = [], []
    for number, chunk in enumerate(chunks):
        index, rest = chunk[:2]
        gathered = [exchange(part) for part in sent[number]]
        gathered = gathered[0] if len(gathered) == 1 else jnp.concatenate(gathered, axis=3)
        coeff_part, value, back = owner_pass(gathered[:, :, :, :cycle_dev], index * LANES, LANES)
        coeff_parts.append(coeff_part)
        partial_value = partial_value + value
        row_pad = groups * GROUP - cycle_dev
        if row_pad:
            back = jnp.pad(back, ((0, 0),) * 3 + ((0, row_pad), (0, 0)))
        pieces = [back[:, :, :, span[0] * GROUP : span[1] * GROUP] for span in spans_back[number]]
        if rest:
            per_row = LANES // rest
            lead = gathered.shape[:3]
            packed = gathered[:, :, :, groups * GROUP :, : per_row * rest]
            unpacked = packed.reshape(lead + (GROUP * per_row, rest))[:, :, :, :cycle_dev]
            coeff_part, value, back_rest = owner_pass(unpacked, col_count - rest, rest)
            coeff_parts.append(coeff_part)
            partial_value = partial_value + value
            back_rest = jnp.pad(back_rest, ((0, 0),) * 3 + ((0, GROUP * per_row - cycle_dev), (0, 0)))
            back_rest = back_rest.reshape(lead + (GROUP, per_row * rest))
            spare = LANES - per_row * rest
            back_rest = jnp.pad(back_rest, ((0, 0),) * 4 + ((0, spare),))
            if number == last and spare >= SPLIT:
                loss_lane = per_row * rest
                back_rest = place_terms(back_rest, split_terms(partial_value), loss_lane)
            pieces[0] = jnp.concatenate([pieces[0], back_rest], axis=3)
        backs.append(pieces)
    coeff_out = jnp.concatenate(coeff_parts, axis=0)
    coeff_out = coeff_out.reshape(1, batch_size, chan_count, 2, wave_dev, degree_count)
    fields = []
    steps = [
        (chunk, part, span, backs[number][part])
        for number, chunk in enumerate(chunks)
        for part, span in enumerate(spans_back[number])
    ]
    returned_rest = None
    for chunk, part, span, back in steps:
        returned = exchange(back)
        returned_rest = returned if part == 0 else returned_rest
        if loss_lane is not None and chunk[1] and part == 0:
            row = returned.shape[3] - GROUP
            terms = returned[:, 0, 0, row, loss_lane : loss_lane + SPLIT]
            partial_value = jnp.sum(terms.astype(jnp.float32))
        fields = list(
            adjoint_dft(
                returned, returned_rest, fields, lengths, phasors, grid3.shape, wave_count, wave_pad,
                scale_row, chunk, span,
            )
        )
        if chunk is chunks[last] and part == 0:
            fields[0], partial_value = lax.optimization_barrier((fields[0], partial_value))
            loss_sum = lax.psum(partial_value, "fld" if loss_lane is not None else ("lat", "fld"))
            fields[0], loss_sum = lax.optimization_barrier((fields[0], loss_sum))
    field = fields[0]
    if chunks[last][1]:
        rest = chunks[last][1]
        field = lax.dynamic_update_slice(field, fields[1][:rest], (col_count - rest, 0, 0))
    term_count = STEPS * col_count * wave_count * (wave_count + 1) // 2
    loss = loss_sum / jnp.float32(term_count)
    return (
        coeff_out,
        loss,
        field.reshape(1, batch_size, chan_count, cycle_dev, segment),
    )


def solution(mesh):
    return jax.shard_map(
        device_program,
        mesh=mesh,
        in_specs=(
            P("fld", None, None, "lat", None),
            P(),
            P(),
            P(),
            P("lat", None, None),
            P("fld", None, None, None, "lat", None),
            P("fld"),
            P(),
        ),
        out_specs=(P("fld", None, None, None, "lat", None), P(), P("fld", None, None, "lat", None)),
        check_vma=False,
    )
```

```python
import functools
import math

import jax
import jax.numpy as jnp
from jax import lax
from jax.experimental import pallas as pl
from jax.experimental.pallas import tpu as pltpu
from jax.sharding import PartitionSpec as P


STEPS = 2
KB = 256
BASE = 128
BITS = 7
GROUP = 8
LANES = 128
SPLIT = 3


def round_up(value, unit):
    return (value + unit - 1) // unit * unit


def phasor_rows(lengths, wave_ids, block_count, wave_pad):
    exponents = [1 << bit for bit in range(BITS)] + [BASE * at for at in range(block_count * (KB // BASE))]
    exponents = jnp.asarray(exponents, dtype=jnp.int32)
    length = lengths[:, None, None]
    length_f = length.astype(jnp.float32)
    product = (exponents[None, :, None] * wave_ids[None, None, :]).astype(jnp.float32)
    inverse = 1.0 / length_f
    phase = product - jnp.floor(product * inverse) * length_f
    phase = jnp.where(phase < 0.0, phase + length_f, phase)
    phase = jnp.where(phase >= length_f, phase - length_f, phase)
    turn = phase * inverse
    quarter = jnp.floor(turn * 4.0 + 0.5)
    x = (turn - 0.25 * quarter) * jnp.float32(2.0 * math.pi)
    x2 = x * x
    sin_x = x * (1.0 + x2 * (-1.0 / 6 + x2 * (1.0 / 120 + x2 * (-1.0 / 5040 + x2 * (1.0 / 362880)))))
    cos_x = 1.0 + x2 * (
        -0.5 + x2 * (1.0 / 24 + x2 * (-1.0 / 720 + x2 * (1.0 / 40320 + x2 * (-1.0 / 3628800))))
    )
    odd = (quarter == 1.0) | (quarter == 3.0)
    cos_t = jnp.where(odd, sin_x, cos_x)
    cos_t = jnp.where((quarter == 1.0) | (quarter == 2.0), -cos_t, cos_t)
    sin_t = jnp.where(odd, cos_x, sin_x)
    sin_t = jnp.where((quarter == 2.0) | (quarter == 3.0), -sin_t, sin_t)
    scale = jnp.where(2 * wave_ids[None, None, :] < length, lax.rsqrt(length_f), jnp.float32(0.0))
    lane_pad = ((0, 0), (0, 0), (0, wave_pad - wave_ids.shape[0]))
    cos_t = jnp.concatenate([cos_t, scale], axis=1)
    sin_t = jnp.concatenate([-sin_t, jnp.zeros_like(scale)], axis=1)
    rows = jnp.concatenate([jnp.pad(cos_t, lane_pad), jnp.pad(sin_t, lane_pad)], axis=2)
    row_pad = round_up(rows.shape[1], 8) - rows.shape[1]
    return jnp.pad(rows, ((0, 0), (0, row_pad), (0, 0)))


def rotate(cos_a, sin_a, cos_b, sin_b):
    return cos_a * cos_b - sin_a * sin_b, cos_a * sin_b + sin_a * cos_b


def build_base(ph_ref, base_ref, slot, wave_pad, scale_row):
    row = lax.broadcasted_iota(jnp.int32, (8, wave_pad), 0)
    cos_v = jnp.broadcast_to(ph_ref[slot, scale_row : scale_row + 1, :wave_pad], (8, wave_pad))
    sin_v = jnp.zeros((8, wave_pad), jnp.float32)
    for bit in range(3):
        on = ((row >> bit) & 1) == 1
        cos_b = jnp.where(on, ph_ref[slot, bit : bit + 1, :wave_pad], 1.0)
        sin_b = jnp.where(on, ph_ref[slot, bit : bit + 1, wave_pad:], 0.0)
        cos_v, sin_v = rotate(cos_v, sin_v, cos_b, sin_b)
    base_ref[0:8, :wave_pad] = cos_v
    base_ref[0:8, wave_pad:] = sin_v
    size, bit = 8, 3
    while size < BASE:
        cos_b = ph_ref[slot, bit : bit + 1, :wave_pad]
        sin_b = ph_ref[slot, bit : bit + 1, wave_pad:]
        for start in range(0, size, 32):
            stop = min(start + 32, size)
            cos_v, sin_v = rotate(
                base_ref[start:stop, :wave_pad], base_ref[start:stop, wave_pad:], cos_b, sin_b
            )
            base_ref[size + start : size + stop, :wave_pad] = cos_v
            base_ref[size + start : size + stop, wave_pad:] = sin_v
        size, bit = size * 2, bit + 1


def table_block(ph_ref, base_ref, table_ref, slot, block, wave_pad):
    for half in range(KB // BASE):
        turn = ph_ref[slot, pl.ds(BITS + block * (KB // BASE) + half, 1), :]
        cos_b, sin_b = turn[:, :wave_pad], turn[:, wave_pad:]
        for start in range(0, BASE, 32):
            cos_v, sin_v = rotate(
                base_ref[start : start + 32, :wave_pad], base_ref[start : start + 32, wave_pad:], cos_b, sin_b
            )
            rows = slice(half * BASE + start, half * BASE + start + 32)
            table_ref[rows, :wave_pad] = cos_v.astype(jnp.bfloat16)
            table_ref[rows, wave_pad:] = sin_v.astype(jnp.bfloat16)


def forward_kernel(
    wave_count, wave_pad, scale_row, first, groups, rest, len_ref, ph_ref, *refs
):
    if rest:
        grid_ref, grid_rest_ref, out_ref, base_ref, table_ref, wide_ref, acc_ref, rows_ref, wide_rest_ref, rest_ref = refs
        rest_cols = grid_rest_ref.shape[0]
        per_row = LANES // rest
        rest_rows = rest_ref.shape[0] // (2 * wave_count)
    else:
        grid_ref, out_ref, base_ref, table_ref, wide_ref, acc_ref, rows_ref = refs
        rest_cols = 0
    group = pl.program_id(0)
    segment = grid_ref.shape[2]
    owners, _, wave_dev = out_ref.shape[:3]

    def store_rows(source):
        for part in range(2):
            rows = source[part * wave_count * GROUP : (part + 1) * wave_count * GROUP, :]
            out_ref[:, part] = rows.reshape(owners, wave_dev, GROUP, LANES).astype(jnp.bfloat16)

    def run_group():
        for lane in range(segment // LANES):
            piece = grid_ref[:, :, lane * LANES : (lane + 1) * LANES].astype(jnp.float32)
            wide_ref[lane] = piece.reshape(LANES * GROUP, LANES)
            if rest:
                piece = grid_rest_ref[:, :, lane * LANES : (lane + 1) * LANES].astype(jnp.float32)
                wide_rest_ref[lane] = piece.reshape(rest_cols * GROUP, LANES)

        def per_slot(slot, carry):
            length = len_ref[(first + group) * GROUP + slot]
            build_base(ph_ref, base_ref, slot, wave_pad, scale_row)
            acc_ref[...] = jnp.zeros_like(acc_ref)

            def per_block(block, inner):
                table_block(ph_ref, base_ref, table_ref, slot, block, wave_pad)
                pieces = []
                for part in range(KB // LANES):
                    lane_block = block * (KB // LANES) + part
                    values = wide_ref[lane_block, pl.ds(slot, LANES, stride=GROUP), :]
                    if rest:
                        extra = wide_rest_ref[lane_block, pl.ds(slot, rest_cols, stride=GROUP), :]
                        values = jnp.concatenate([values, extra], axis=0)
                    at = lane_block * LANES + lax.broadcasted_iota(jnp.int32, values.shape, 1)
                    pieces.append(jnp.where(at < length, values, 0.0).astype(jnp.bfloat16))
                acc_ref[...] += jnp.dot(
                    jnp.concatenate(pieces, axis=1), table_ref[...], preferred_element_type=jnp.float32
                )
                return inner

            lax.fori_loop(0, (length + KB - 1) // KB, per_block, 0)
            for part in range(2):
                lanes = slice(part * wave_pad, (part + 1) * wave_pad)
                turned = acc_ref[:LANES, lanes].T
                rows_ref[pl.ds(part * wave_count * GROUP + slot, wave_count, stride=GROUP), :] = (
                    turned[:wave_count]
                )
                if rest:
                    cycle = (first + group) * GROUP + slot
                    turned = acc_ref[LANES:, lanes].T[:wave_count]
                    fill = jnp.zeros((wave_count, LANES - rest_cols), jnp.float32)
                    turned = jnp.concatenate([turned, fill], axis=1)
                    keep = lax.broadcasted_iota(jnp.int32, turned.shape, 1) < rest
                    turned = jnp.where(keep, turned, 0.0)
                    turned = pltpu.roll(turned, lax.rem(cycle, per_row) * rest, 1)
                    at = pl.ds(part * wave_count * rest_rows + cycle // per_row, wave_count, stride=rest_rows)
                    rest_ref[at, :] += turned
            return carry

        lax.fori_loop(0, GROUP, per_slot, 0)
        store_rows(rows_ref)

    if rest:

        @pl.when(group == 0)
        def _():
            rest_ref[...] = jnp.zeros_like(rest_ref)

        pl.when(group < groups)(run_group)

        @pl.when(group == groups)
        def _():
            store_rows(rest_ref)
    else:
        run_group()


def forward_dft(grid, lengths, phasors, owners, wave_count, wave_pad, scale_row, chunk, span):
    index, rest, rest_cols, rest_index = chunk
    _, _, segment = grid.shape
    first, groups = span[0], span[1] - span[0]
    wide_lanes = round_up(segment, KB) // LANES
    wave_dev = wave_count // owners
    rows = (groups + (1 if rest else 0)) * GROUP
    last = span[1] - 1
    in_specs = [
        pl.BlockSpec((GROUP,) + phasors.shape[1:], lambda g, n: (jnp.minimum(first + g, last), 0, 0)),
        pl.BlockSpec((LANES, GROUP, segment), lambda g, n: (index, jnp.minimum(first + g, last), 0)),
    ]
    operands = [lengths, phasors, grid]
    scratch = [
        pltpu.VMEM((BASE, 2 * wave_pad), jnp.float32),
        pltpu.VMEM((KB, 2 * wave_pad), jnp.bfloat16),
        pltpu.VMEM((wide_lanes, LANES * GROUP, LANES), jnp.float32),
        pltpu.VMEM((LANES + rest_cols, 2 * wave_pad), jnp.float32),
        pltpu.VMEM((2 * wave_count * GROUP, LANES), jnp.float32),
    ]
    if rest:
        in_specs.append(
            pl.BlockSpec((rest_cols, GROUP, segment), lambda g, n: (rest_index, jnp.minimum(first + g, last), 0))
        )
        operands.append(grid)
        scratch += [
            pltpu.VMEM((wide_lanes, rest_cols * GROUP, LANES), jnp.float32),
            pltpu.VMEM((2 * wave_count * GROUP, LANES), jnp.float32),
        ]
    return pl.pallas_call(
        functools.partial(forward_kernel, wave_count, wave_pad, scale_row, first, groups, rest),
        out_shape=jax.ShapeDtypeStruct((owners, 2, wave_dev, rows, LANES), jnp.bfloat16),
        grid_spec=pltpu.PrefetchScalarGridSpec(
            num_scalar_prefetch=1,
            grid=(rows // GROUP,),
            in_specs=in_specs,
            out_specs=pl.BlockSpec((owners, 2, wave_dev, GROUP, LANES), lambda g, n: (0, 0, 0, g, 0)),
            scratch_shapes=scratch,
        ),
        compiler_params=pltpu.CompilerParams(
            dimension_semantics=("arbitrary",), vmem_limit_bytes=56 * 1024 * 1024
        ),
        cost_estimate=pl.CostEstimate(
            flops=2 * LANES * groups * GROUP * segment * wave_pad,
            bytes_accessed=2 * LANES * groups * GROUP * (segment + 2 * wave_count),
            transcendentals=0,
        ),
        name="forward_dft",
    )(*operands)


def adjoint_kernel(wave_count, wave_pad, scale_row, first, rest, aliased, len_ref, ph_ref, *refs):
    refs = list(refs)
    back_ref = refs.pop(0)
    back_rest_ref = refs.pop(0) if rest else None
    del refs[:aliased]
    out_ref = refs.pop(0)
    out_rest_ref = refs.pop(0) if rest else None
    base_ref, table_ref, lhs_ref, rows_ref, wide_ref = refs[:5]
    if rest:
        wide_rest_ref, rest_ref = refs[5:]
        rest_cols = out_rest_ref.shape[0]
        per_row = LANES // rest
    group = pl.program_id(0)
    segment = out_ref.shape[2]
    lane_count = wide_ref.shape[0]
    per_kb = KB // LANES
    span = wave_count * GROUP
    for part in range(2):
        rows_ref[part * span : (part + 1) * span, :] = (
            back_ref[:, part].astype(jnp.float32).reshape(span, LANES)
        )

    @pl.when(group == 0)
    def _():
        lhs_ref[...] = jnp.zeros_like(lhs_ref)
        if rest:
            for part in range(2):
                rest_ref[part * span : (part + 1) * span, :] = (
                    back_rest_ref[:, part].astype(jnp.float32).reshape(span, LANES)
                )

    def put(slot, lane_block, values):
        wide_ref[lane_block, pl.ds(slot, LANES, stride=GROUP), :] = values[:LANES]
        if rest:
            wide_rest_ref[lane_block, pl.ds(slot, rest_cols, stride=GROUP), :] = values[LANES:]

    def per_slot(slot, carry):
        length = len_ref[(first + group) * GROUP + slot]
        build_base(ph_ref, base_ref, slot, wave_pad, scale_row)
        for part in range(2):
            lanes = slice(part * wave_pad, part * wave_pad + wave_count)
            turned = rows_ref[pl.ds(part * span + slot, wave_count, stride=GROUP), :].T
            lhs_ref[:LANES, lanes] = turned.astype(jnp.bfloat16)
            if rest:
                cycle = (first + group) * GROUP + slot
                rows = rest_ref[pl.ds(part * span + cycle // per_row, wave_count, stride=GROUP), :]
                rows = pltpu.roll(rows, LANES - lax.rem(cycle, per_row) * rest, 1)
                lhs_ref[LANES:, lanes] = rows[:, :rest_cols].T.astype(jnp.bfloat16)
        used = (length + KB - 1) // KB

        def per_block(block, inner):
            table_block(ph_ref, base_ref, table_ref, slot, block, wave_pad)
            values = lax.dot_general(
                lhs_ref[...], table_ref[...], (((1,), (1,)), ((), ())), preferred_element_type=jnp.float32
            )
            for part in range(per_kb):
                lane_block = block * per_kb + part
                piece = values[:, part * LANES : (part + 1) * LANES]
                at = lane_block * LANES + lax.broadcasted_iota(jnp.int32, piece.shape, 1)
                put(slot, lane_block, jnp.where(at < length, piece, 0.0))
            return inner

        def fill(lane_block, inner):
            put(slot, lane_block, jnp.zeros((lhs_ref.shape[0], LANES), jnp.float32))
            return inner

        lax.fori_loop(0, used, per_block, 0)
        lax.fori_loop(used * per_kb, lane_count, fill, 0)
        return carry

    lax.fori_loop(0, GROUP, per_slot, 0)
    for lane in range(segment // LANES):
        lanes = slice(lane * LANES, (lane + 1) * LANES)
        out_ref[:, :, lanes] = wide_ref[lane].reshape(LANES, GROUP, LANES).astype(jnp.bfloat16)
        if rest:
            values = wide_rest_ref[lane].reshape(rest_cols, GROUP, LANES)
            out_rest_ref[:, :, lanes] = values.astype(jnp.bfloat16)


def adjoint_dft(back, back_rest, fields, lengths, phasors, out_shape, wave_count, wave_pad, scale_row, chunk, span):
    index, rest, rest_cols, _ = chunk
    _, cycle_dev, segment = out_shape
    owners, _, wave_dev, _, _ = back.shape
    first, groups = span[0], span[1] - span[0]
    wide_lanes = round_up(segment, KB) // LANES
    aliased = len(fields)
    block = (owners, 2, wave_dev, GROUP, LANES)
    in_specs = [
        pl.BlockSpec((GROUP,) + phasors.shape[1:], lambda g, n: (first + g, 0, 0)),
        pl.BlockSpec(block, lambda g, n: (0, 0, 0, g, 0)),
    ]
    operands = [lengths, phasors, back]
    out_specs = [pl.BlockSpec((LANES, GROUP, segment), lambda g, n: (index, first + g, 0))]
    out_shapes = [jax.ShapeDtypeStruct(out_shape, jnp.bfloat16)]
    scratch = [
        pltpu.VMEM((BASE, 2 * wave_pad), jnp.float32),
        pltpu.VMEM((KB, 2 * wave_pad), jnp.bfloat16),
        pltpu.VMEM((LANES + rest_cols, 2 * wave_pad), jnp.bfloat16),
        pltpu.VMEM((2 * wave_count * GROUP, LANES), jnp.float32),
        pltpu.VMEM((wide_lanes, LANES * GROUP, LANES), jnp.float32),
    ]
    if rest:
        rest_block = back_rest.shape[3] // GROUP - 1
        in_specs.append(pl.BlockSpec(block, lambda g, n: (0, 0, 0, rest_block, 0)))
        operands.append(back_rest)
        out_specs.append(pl.BlockSpec((rest_cols, GROUP, segment), lambda g, n: (0, first + g, 0)))
        out_shapes.append(jax.ShapeDtypeStruct((rest_cols, cycle_dev, segment), jnp.bfloat16))
        scratch += [
            pltpu.VMEM((wide_lanes, rest_cols * GROUP, LANES), jnp.float32),
            pltpu.VMEM((2 * wave_count * GROUP, LANES), jnp.float32),
        ]
    aliases = {}
    for output, field in enumerate(fields):
        aliases[len(operands)] = output
        in_specs.append(pl.BlockSpec(memory_space=pl.ANY))
        operands.append(field)
    return pl.pallas_call(
        functools.partial(adjoint_kernel, wave_count, wave_pad, scale_row, first, rest, aliased),
        out_shape=out_shapes,
        grid_spec=pltpu.PrefetchScalarGridSpec(
            num_scalar_prefetch=1, grid=(groups,), in_specs=in_specs, out_specs=out_specs, scratch_shapes=scratch
        ),
        input_output_aliases=aliases,
        compiler_params=pltpu.CompilerParams(
            dimension_semantics=("arbitrary",), vmem_limit_bytes=60 * 1024 * 1024
        ),
        cost_estimate=pl.CostEstimate(
            flops=2 * LANES * groups * GROUP * segment * wave_pad,
            bytes_accessed=2 * LANES * groups * GROUP * (segment + 2 * wave_count),
            transcendentals=0,
        ),
        name="adjoint_dft",
    )(*operands)


def split_terms(value):
    terms = []
    for _ in range(SPLIT):
        term = lax.reduce_precision(value, exponent_bits=8, mantissa_bits=7)
        terms.append(term.astype(jnp.bfloat16))
        value = value - term
    return terms


def place_terms(rows, terms, lane):
    at = [lax.broadcasted_iota(jnp.int32, rows.shape, axis) for axis in range(1, rows.ndim)]
    first = (at[0] == 0) & (at[1] == 0) & (at[2] == 0)
    for number, term in enumerate(terms):
        rows = jnp.where(first & (at[3] == lane + number), term, rows)
    return rows


def column_chunks(col_count):
    whole = col_count // LANES
    rest = col_count - whole * LANES
    chunks = [(index, 0, 0, 0) for index in range(whole)]
    if rest:
        width = 8
        while width < rest:
            width *= 2
        chunks[-1] = (whole - 1, rest, width, whole * LANES // width)
    return chunks


def device_program(grid, cycle_ids, cycle_len, wave_ids, legendre, target, step_w, chan_w):
    _, batch_size, chan_count, cycle_dev, segment = grid.shape
    wave_count = wave_ids.shape[0]
    wave_dev, degree_count, _ = legendre.shape
    owners = wave_count // wave_dev
    col_count = batch_size * chan_count
    wave_pad = round_up(wave_count, LANES)
    block_count = pl.cdiv(segment, KB)
    scale_row = BITS + block_count * (KB // BASE)
    lat_index = lax.axis_index("lat")
    my_cycles = lax.dynamic_slice_in_dim(cycle_ids, lat_index * cycle_dev, cycle_dev)
    lengths = jnp.take(cycle_len, my_cycles)
    phasors = phasor_rows(lengths, wave_ids, block_count, wave_pad)
    group_pad = round_up(cycle_dev, GROUP) - cycle_dev
    if group_pad:
        lengths = jnp.pad(lengths, (0, group_pad))
        phasors = jnp.pad(phasors, ((0, group_pad), (0, 0), (0, 0)))
    grid3 = grid.reshape(col_count, cycle_dev, segment)
    my_waves = lax.dynamic_slice_in_dim(wave_ids, lat_index * wave_dev, wave_dev)
    degree = jnp.arange(degree_count, dtype=jnp.int32)
    kept = (degree[None, :] >= my_waves[:, None]).astype(jnp.float32)[:, :, None, None]
    factor = jnp.where(my_waves == 0, 1.0, 2.0).astype(jnp.float32)
    weight_cols = jnp.broadcast_to(step_w[0] * chan_w[None, :], (batch_size, chan_count)).reshape(
        col_count
    )
    target3 = target.reshape(col_count, 2, wave_dev, degree_count)

    def exchange(values):
        shape = values.shape
        flat = values.reshape((owners * 2 * wave_dev,) + shape[3:])
        return lax.all_to_all(flat, "lat", split_axis=0, concat_axis=0, tiled=True).reshape(shape)

    chunks = column_chunks(col_count)
    groups = pl.cdiv(cycle_dev, GROUP)
    last = len(chunks) - 1
    head = tail = max(1, 2 * groups // 5)
    spans_out = [[(0, groups)] for _ in chunks]
    spans_back = [[(0, groups)] for _ in chunks]
    if groups > 1:
        spans_out[0] = [(0, head), (head, groups)]
        spans_back[last] = [(0, groups - tail), (groups - tail, groups)]
    sent = []
    for number, chunk in enumerate(chunks):
        parts = []
        for span in spans_out[number]:
            rides = chunk if span[1] == groups else (chunk[0], 0, 0, 0)
            part = forward_dft(
                grid3, lengths, phasors, owners, wave_count, wave_pad, scale_row, rides, span
            )
            part, lengths, legendre, target3 = lax.optimization_barrier((part, lengths, legendre, target3))
            parts.append(part)
        sent.append(parts)
    legendre_cols = jnp.take(legendre, cycle_ids, axis=2).reshape(
        wave_dev, degree_count, owners, cycle_dev
    )

    def owner_pass(gathered, start, cols):
        coeffs = jnp.einsum(
            "sndp,dtspc->sntc", legendre_cols, gathered, preferred_element_type=jnp.float32
        )
        coeffs = coeffs * kept
        goal = jnp.transpose(target3[start : start + cols], (2, 3, 1, 0))
        weight = factor[:, None, None, None] * weight_cols[None, None, None, start : start + cols]
        misfit = (coeffs - goal) * kept
        value = jnp.sum(weight * misfit * misfit)
        grad_coeff = (2.0 * weight * misfit).astype(jnp.bfloat16)
        back = jnp.einsum(
            "sndp,sntc->dtspc", legendre_cols, grad_coeff, preferred_element_type=jnp.float32
        ).astype(jnp.bfloat16)
        return jnp.transpose(coeffs, (3, 2, 0, 1)), value, back

    partial_value = jnp.float32(0.0)
    loss_lane = None
    coeff_parts, backs = [], []
    for number, chunk in enumerate(chunks):
        index, rest = chunk[:2]
        gathered = [exchange(part) for part in sent[number]]
        gathered = gathered[0] if len(gathered) == 1 else jnp.concatenate(gathered, axis=3)
        coeff_part, value, back = owner_pass(gathered[:, :, :, :cycle_dev], index * LANES, LANES)
        coeff_parts.append(coeff_part)
        partial_value = partial_value + value
        row_pad = groups * GROUP - cycle_dev
        if row_pad:
            back = jnp.pad(back, ((0, 0),) * 3 + ((0, row_pad), (0, 0)))
        pieces = [back[:, :, :, span[0] * GROUP : span[1] * GROUP] for span in spans_back[number]]
        if rest:
            per_row = LANES // rest
            lead = gathered.shape[:3]
            packed = gathered[:, :, :, groups * GROUP :, : per_row * rest]
            unpacked = packed.reshape(lead + (GROUP * per_row, rest))[:, :, :, :cycle_dev]
            coeff_part, value, back_rest = owner_pass(unpacked, col_count - rest, rest)
            coeff_parts.append(coeff_part)
            partial_value = partial_value + value
            back_rest = jnp.pad(back_rest, ((0, 0),) * 3 + ((0, GROUP * per_row - cycle_dev), (0, 0)))
            back_rest = back_rest.reshape(lead + (GROUP, per_row * rest))
            spare = LANES - per_row * rest
            back_rest = jnp.pad(back_rest, ((0, 0),) * 4 + ((0, spare),))
            if number == last and spare >= SPLIT:
                loss_lane = per_row * rest
                back_rest = place_terms(back_rest, split_terms(partial_value), loss_lane)
            pieces[0] = jnp.concatenate([pieces[0], back_rest], axis=3)
        backs.append(pieces)
    coeff_out = jnp.concatenate(coeff_parts, axis=0)
    coeff_out = coeff_out.reshape(1, batch_size, chan_count, 2, wave_dev, degree_count)
    fields = []
    steps = [
        (chunk, part, span, backs[number][part])
        for number, chunk in enumerate(chunks)
        for part, span in enumerate(spans_back[number])
    ]
    returned_rest = None
    for chunk, part, span, back in steps:
        returned = exchange(back)
        returned_rest = returned if part == 0 else returned_rest
        if loss_lane is not None and chunk[1] and part == 0:
            row = returned.shape[3] - GROUP
            terms = returned[:, 0, 0, row, loss_lane : loss_lane + SPLIT]
            partial_value = jnp.sum(terms.astype(jnp.float32))
        fields = list(
            adjoint_dft(
                returned, returned_rest, fields, lengths, phasors, grid3.shape, wave_count, wave_pad,
                scale_row, chunk, span,
            )
        )
        if chunk is chunks[last] and part == 0:
            fields[0], partial_value = lax.optimization_barrier((fields[0], partial_value))
            loss_sum = lax.psum(partial_value, "fld" if loss_lane is not None else ("lat", "fld"))
            fields[0], loss_sum = lax.optimization_barrier((fields[0], loss_sum))
    field = fields[0]
    if chunks[last][1]:
        rest = chunks[last][1]
        field = lax.dynamic_update_slice(field, fields[1][:rest], (col_count - rest, 0, 0))
    term_count = STEPS * col_count * wave_count * (wave_count + 1) // 2
    loss = loss_sum / jnp.float32(term_count)
    return (
        coeff_out,
        loss,
        field.reshape(1, batch_size, chan_count, cycle_dev, segment),
    )


def solution(mesh):
    return jax.shard_map(
        device_program,
        mesh=mesh,
        in_specs=(
            P("fld", None, None, "lat", None),
            P(),
            P(),
            P(),
            P("lat", None, None),
            P("fld", None, None, None, "lat", None),
            P("fld"),
            P(),
        ),
        out_specs=(P("fld", None, None, None, "lat", None), P(), P("fld", None, None, "lat", None)),
        check_vma=False,
    )
```
